128 devices in a mesh: blk: 64 (over x, y, z_lo, core), grp: 2 (over z_hi).
Axes of the slice: x: 4, y: 4, z: 4 (z_hi: 2, z_lo: 2; z = z_hi * 2 + z_lo), core: 2. Of those that a mesh axis runs over, the one named last changes fastest.
Arguments:
- sky_maps: float32 [4, 512, 4096], P(None, ('blk', 'grp')), may hold values from -6 to 6
- legendre: bfloat16 [512, 512, 2048], P(('blk', 'grp')), may hold values from -0.25 to 0.25
- owner_table: int32 [512], replicated, may hold values from 0 to 511, each once
Outputs:
- harmonics: float32 [512, 4, 2, 2048], P(('blk', 'grp'))
- spectra: float32 [10, 2048], P(None, ('blk', 'grp'))
The draws below stay inside these ranges and needn't reach their ends.
Inputs may be any that keep to these rules, and one draw needn't show every extreme that they name: `owner_table`: a permutation of the orders 0 to 511.
All inputs are finite; a program needn't handle non-finite values.
Results may differ from the reference program's by a relative error of at most 0.0034.
Values may be sent and summed in bfloat16 or wider, within the bound.
No kernel may reach another device: no remote copies, remote signals or barrier semaphores. Data moves between devices by JAX's collectives and lax.ppermute only.
A program may use at most 128 MiB of HBM per device.

```python
import math
import jax
import jax.numpy as jnp
import numpy as np
from jax import lax

MAPS = 4
M = 512
L = 2048
NPHI = 4096
CYCLES = 512


def levels(own_key, shape, shards, smallest, top_value):
    def one(dim, blocks):
        heights = jax.random.uniform(jax.random.fold_in(jax.random.fold_in(own_key, 6), dim), (blocks,), jnp.float32, smallest / len(shards), top_value / len(shards))
        return jnp.repeat(jnp.exp(heights), shape[dim] // blocks).reshape((-1,) + (1,) * (len(shape) - dim - 1))

    loudness = one(*shards[0])
    for cut in shards[1:]:
        loudness = loudness * one(*cut)
    return loudness


def scatter_about(own_key, dims, scale, limit, pieces=(), kind=jnp.bfloat16):
    array = scale * jax.random.normal(own_key, dims, jnp.float32)
    if pieces:
        array = array * levels(own_key, dims, pieces, -0.22, 0.18)
    return jnp.clip(array, -limit, limit).astype(kind)


def setup_inputs(seed: int = 0) -> dict:
    seeds = jax.random.split(jax.random.key(seed), 4)
    sky_maps = scatter_about(seeds[0], (MAPS, CYCLES, NPHI), 1.0, 6.0, ((1, 128),), jnp.float32)
    legendre = scatter_about(seeds[1], (CYCLES, M, L), CYCLES ** -0.5, 0.25, ((0, 128),))
    owner_table = jax.random.permutation(seeds[2], M).astype(jnp.int32)
    return dict(sky_maps=sky_maps, legendre=legendre, owner_table=owner_table)


def reference(sky_maps, legendre, owner_table):
    coeffs = jnp.fft.rfft(sky_maps, axis=-1)[..., :M] / math.sqrt(NPHI)
    fourier = jnp.stack([jnp.real(coeffs), jnp.imag(coeffs)], axis=2)
    fourier = jnp.transpose(fourier, (1, 0, 2, 3)).reshape(CYCLES, 2 * MAPS, M).astype(jnp.bfloat16)
    ell_index = jnp.arange(L, dtype=jnp.int32)

    def per_block(orders):
        table = jnp.take(legendre, orders, axis=1).astype(jnp.float32)
        values = jnp.take(fourier, orders, axis=2).astype(jnp.float32)
        block = jnp.einsum('rcm,rml->mcl', values, table)
        keep = ell_index[None, None, :] >= orders[:, None, None]
        return jnp.where(keep, block, jnp.zeros_like(block))
    harmonics = lax.map(per_block, owner_table.reshape(M // 64, 64)).reshape(M, MAPS, 2, L)
    weight = jnp.where(owner_table == 0, jnp.float32(1.0), jnp.float32(2.0)).astype(jnp.float32)
    cross = jnp.einsum('m,miql,mjql->ijl', weight, harmonics, harmonics)
    first, second = np.triu_indices(MAPS)
    spectra = cross[first, second] / (2 * ell_index + 1).astype(jnp.float32)
    return (harmonics, spectra)
```

```python
import functools
import math

import jax
import jax.numpy as jnp
import numpy as np
from jax import lax
from jax.experimental import pallas as pl
from jax.experimental.pallas import tpu as pltpu
from jax.sharding import Mesh
from jax.sharding import PartitionSpec as P

BLK_GRP = ("blk_0", "blk_1", "blk_2", "blk_3", "grp")
X, Y, Z, CORE = "blk_0", "blk_1", "z", "blk_3"
COLOURS = (
    (0, 768, ((X, Y, Z), (Y, Z, X))),
    (768, 256, ((Z, X, Y), (Z, X, Y))),
)
SHIFTS = (2, 1, 3)
F32, BF16 = jnp.float32, jnp.bfloat16
SMEM = pl.BlockSpec(memory_space=pltpu.SMEM)
VMEM = pl.BlockSpec(memory_space=pltpu.VMEM)
ANY = pl.BlockSpec(memory_space=pl.ANY)


def places(device):
    return {
        X: device // 32,
        Y: device // 8 % 4,
        Z: device % 2 * 2 + device // 4 % 2,
        CORE: device // 2 % 2,
    }


def index_of(place):
    z = place[Z]
    return place[X] * 32 + place[Y] * 8 + z % 2 * 4 + place[CORE] * 2 + z // 2


def shift_along(x, axes, shift):
    pairs = []
    for device in range(128):
        place = places(device)
        axis = axes[place[CORE]]
        pairs.append((device, index_of({**place, axis: (place[axis] + shift) % 4})))
    return lax.ppermute(x, BLK_GRP, pairs)


def swap_cores(x):
    return lax.ppermute(x, CORE, [(0, 1), (1, 0)])


def half_kernel(first, width, core_ref, leg_ref, out_ref, sem):
    start = pl.multiple_of((1 - core_ref[0]) * 1024 + first, 128)
    copy = pltpu.make_async_copy(leg_ref.at[:, :, pl.ds(start, width)], out_ref, sem)
    copy.start()
    copy.wait()


def other_half(first, width, core, legendre):
    return pl.pallas_call(
        functools.partial(half_kernel, first, width),
        name=f"other_half_{first}",
        out_shape=jax.ShapeDtypeStruct((4, 512, width), BF16),
        in_specs=[SMEM, ANY],
        out_specs=VMEM,
        scratch_shapes=[pltpu.SemaphoreType.DMA],
        cost_estimate=pl.CostEstimate(flops=width * 8192, bytes_accessed=width * 8192, transcendentals=0),
    )(core, legendre)


def real_fft(values):
    n = len(values)
    if n == 1:
        return [(values[0], None)]
    even, odd = real_fft(values[0::2]), real_fft(values[1::2])
    half = n // 2
    out = []
    for k in range(half + 1):
        er, ei = pick(even, k % half, half)
        orr, oi = pick(odd, k % half, half)
        c, s = math.cos(2 * math.pi * k / n), math.sin(2 * math.pi * k / n)
        if k == 0:
            tr, ti = orr, oi
        elif 2 * k == n:
            tr, ti = -orr, (None if oi is None else -oi)
        elif 4 * k == n:
            tr, ti = oi, -orr
        else:
            tr = orr * c if oi is None else orr * c + oi * s
            ti = -orr * s if oi is None else oi * c - orr * s
        out.append((plus(er, tr), plus(ei, ti)))
    return out


def plus(a, b):
    if a is None:
        return b
    return a if b is None else a + b


def pick(spectrum, k, n):
    if k <= n // 2:
        return spectrum[k]
    re, im = spectrum[n - k]
    return re, (None if im is None else -im)


def fourier_kernel(x_ref, cos_ref, sin_ref, tail_ref, out_ref, z_ref):
    part = lax.broadcasted_iota(jnp.int32, (8, 128), 0) % 2
    total = None
    for r in range(4):
        slabs = [x_ref[8 * r : 8 * r + 8, 128 * k : 128 * k + 128] for k in range(32)]
        spectrum = real_fft(slabs)
        for m in range(32):
            re, im = pick(spectrum, m, 32)
            c, s = cos_ref[m : m + 1, :], sin_ref[m : m + 1, :]
            if im is None:
                re, im = re * c, -re * s
            else:
                re, im = re * c + im * s, im * c - re * s
            z_ref[8 * m : 8 * m + 8, 0:128] = jnp.where(part == 0, re, im)
            z_ref[8 * m : 8 * m + 8, 128:256] = jnp.where(part == 0, im, -re)
        out = jnp.dot(z_ref[...], tail_ref[...], precision=lax.Precision.HIGHEST, preferred_element_type=F32)
        out = pltpu.roll(out, 16 * r, 1) if r else out
        total = out if total is None else total + out
    out_ref[...] = (total * (1.0 / 64.0)).astype(BF16)


def fourier_columns(sky_maps):
    maps, cycles, pixels = sky_maps.shape
    rows = jnp.broadcast_to(jnp.transpose(sky_maps, (1, 0, 2))[:, :, None, :], (cycles, maps, 2, pixels))
    rows = rows.reshape(cycles * maps * 2, pixels)
    turn = 2 * np.pi / 4096 * np.outer(np.arange(32), np.arange(128))
    last = 2 * np.pi / 128 * np.outer(np.arange(128), np.arange(16))
    tail = np.zeros((256, 128))
    tail[:128, :16] = np.cos(last)
    tail[128:, :16] = np.sin(last)
    return pl.pallas_call(
        fourier_kernel,
        name="fourier",
        out_shape=jax.ShapeDtypeStruct((256, 128), BF16),
        in_specs=[VMEM] * 4,
        out_specs=VMEM,
        scratch_shapes=[pltpu.VMEM((256, 256), F32)],
        cost_estimate=pl.CostEstimate(flops=400_000_000, bytes_accessed=1 << 20, transcendentals=0),
    )(rows, jnp.asarray(np.cos(turn), F32), jnp.asarray(np.sin(turn), F32), jnp.asarray(tail, F32))


def weights_kernel(own_ref, got_ref, out_ref):
    columns = jnp.concatenate([own_ref[...], got_ref[...]], axis=1)
    k = lax.broadcasted_iota(jnp.int32, (256, 256), 0)
    n = lax.broadcasted_iota(jnp.int32, (256, 256), 1)
    cycle_of = jnp.where(k % 128 < 64, (k // 128) * 4 + (k % 128) // 16, -1)
    spread = jnp.where(cycle_of == n // 32, 1.0, 0.0).astype(BF16)
    keep = jnp.where((k // 8) == (n % 32), 1.0, 0.0).astype(BF16)
    for g in range(16):
        pick_group = jnp.where(n % 16 == g, 1.0, 0.0).astype(BF16)
        spread_out = jnp.dot(columns * pick_group, spread, preferred_element_type=F32)
        out_ref[g] = spread_out.astype(BF16) * keep


def order_weights(own_f, got_f):
    return pl.pallas_call(
        weights_kernel,
        name="order_weights",
        out_shape=jax.ShapeDtypeStruct((16, 256, 256), BF16),
        in_specs=[VMEM] * 2,
        out_specs=VMEM,
        cost_estimate=pl.CostEstimate(flops=1 << 29, bytes_accessed=2 << 20, transcendentals=0),
    )(own_f, got_f)


def chip_sums_kernel(first, width, core_ref, place_ref, leg_ref, got_ref, weights_ref, *rest):
    outs, (table, sums, in_sems, out_sems) = rest[:4], rest[4:]
    start = pl.multiple_of(core_ref[0] * 1024 + first, 128)

    def copies(g):
        rows = slice(g * 32, g * 32 + 32)
        mine = pltpu.make_async_copy(
            leg_ref.at[:, rows, pl.ds(start, width)], table.at[0:4, rows, :], in_sems.at[g, 0]
        )
        other = pltpu.make_async_copy(got_ref.at[:, rows, :], table.at[4:8, rows, :], in_sems.at[g, 1])
        return mine, other

    for g in range(16):
        for copy in copies(g):
            copy.start()
    for g in range(16):
        for copy in copies(g):
            copy.wait()
        values = table[:, g * 32 : g * 32 + 32, :].reshape(256, width)
        done = jnp.dot(weights_ref[g], values, preferred_element_type=F32)
        for m in range(32):
            sums[place_ref[g * 32 + m]] = done[8 * m : 8 * m + 8].astype(BF16)
    out_copies = [
        pltpu.make_async_copy(sums.at[128 * d : 128 * d + 128], outs[d], out_sems.at[d]) for d in range(4)
    ]
    for copy in out_copies:
        copy.start()
    for copy in out_copies:
        copy.wait()


def chip_sums(first, width, core, place, legendre, got, weights):
    return pl.pallas_call(
        functools.partial(chip_sums_kernel, first, width),
        name=f"chip_sums_{first}",
        out_shape=[jax.ShapeDtypeStruct((128, 8, width), BF16)] * 4,
        in_specs=[SMEM, SMEM, ANY, ANY, VMEM],
        out_specs=[ANY] * 4,
        scratch_shapes=[
            pltpu.VMEM((8, 512, width), BF16),
            pltpu.VMEM((512, 8, width), BF16),
            pltpu.SemaphoreType.DMA((16, 2)),
            pltpu.SemaphoreType.DMA((4,)),
        ],
        cost_estimate=pl.CostEstimate(flops=width * 1_000_000, bytes_accessed=width * 16384, transcendentals=0),
    )(core, place, legendre, got, weights)


def add_kernel(own_ref, a_ref, b_ref, c_ref, *outs):
    count = outs[0].shape[0]
    for d, out in enumerate(outs):
        part = pl.ds(d * count, count)
        total = own_ref[part].astype(F32) + a_ref[part].astype(F32)
        total = total + b_ref[part].astype(F32) + c_ref[part].astype(F32)
        out[...] = total.astype(out.dtype)


def add_blocks(parts):
    count, rows, width = parts[0].shape
    return pl.pallas_call(
        add_kernel,
        name="add_blocks",
        out_shape=[jax.ShapeDtypeStruct((count // 4, rows, width), F32 if d == 0 else BF16) for d in range(4)],
        in_specs=[VMEM] * 4,
        out_specs=[VMEM] * 4,
        cost_estimate=pl.CostEstimate(flops=count * width * 64, bytes_accessed=count * width * 80, transcendentals=0),
    )(*parts)


def finish_kernel(core_ref, order_ref, *refs):
    ins, (own_ref, send_ref, cross_ref) = refs[:-3], refs[-3:]
    core = core_ref[0]
    for colour, (first, width, _) in enumerate(COLOURS):
        lane = slice(first, first + width)
        ell = lax.broadcasted_iota(jnp.int32, (8, width), 1) + core * 1024 + first
        totals = [jnp.zeros((8, width), F32) for _ in range(4)]
        parts = ins[4 * colour : 4 * colour + 4]

        def slot_sum(slot):
            h = parts[0][slot].astype(F32) + parts[1][slot].astype(F32)
            h = h + parts[2][slot].astype(F32) + parts[3][slot].astype(F32)
            order = order_ref[slot]
            h = jnp.where(ell >= order, h, 0.0)
            weighted = h * jnp.where(order == 0, 1.0, 2.0)
            for delta in range(4):
                other = pltpu.roll(h, 8 - 2 * delta, 0) if delta else h
                totals[delta] = totals[delta] + weighted * other
            return h

        for j in range(4):
            own_ref[j, :, lane] = slot_sum(core * 4 + j)
            send_ref[j, :, lane] = slot_sum((1 - core) * 4 + j)
        row = 0
        for i in range(4):
            for j in range(i, 4):
                t = totals[j - i]
                cross_ref[row : row + 1, lane] = t[2 * i : 2 * i + 1] + t[2 * i + 1 : 2 * i + 2]
                row += 1


def finish(core, orders, parts):
    return pl.pallas_call(
        finish_kernel,
        name="finish",
        out_shape=[
            jax.ShapeDtypeStruct((4, 8, 1024), F32),
            jax.ShapeDtypeStruct((4, 8, 1024), F32),
            jax.ShapeDtypeStruct((10, 1024), F32),
        ],
        in_specs=[SMEM, SMEM] + [VMEM] * len(parts),
        out_specs=[VMEM] * 3,
        cost_estimate=pl.CostEstimate(flops=8 * 8 * 1024 * 16, bytes_accessed=1 << 20, transcendentals=0),
    )(core, orders, *parts)


def per_device(sky_maps, legendre, owner_table):
    my_index = lax.axis_index(BLK_GRP)
    here = places(my_index)
    core = here[CORE]
    core_scalar = core.reshape(1).astype(jnp.int32)

    received = [swap_cores(other_half(first, width, core_scalar, legendre)) for first, width, _ in COLOURS]
    own_f = fourier_columns(sky_maps)
    weights = order_weights(own_f, swap_cores(own_f))

    slots = lax.iota(jnp.int32, 512)
    slot_of = jnp.sum(jnp.where(owner_table[:, None] == slots[None, :], slots[:, None], 0), axis=0)
    owner = places(slot_of // 4)
    in_chip = owner[CORE] * 4 + slot_of % 4
    apart = {axis: (owner[axis] - here[axis]) % 4 for axis in (X, Y, Z)}

    blocks = []
    for (first, width, axes), got in zip(COLOURS, received):
        a, b, c = (jnp.where(core == 0, apart[axes[0][k]], apart[axes[1][k]]) for k in range(3))
        place = ((a * 4 + b) * 4 + c) * 8 + in_chip
        blocks.append(chip_sums(first, width, core_scalar, place, legendre, got, weights))
    last = []
    for stage in range(3):
        for colour, (_, _, axes) in enumerate(COLOURS):
            sent = blocks[colour]
            now = (axes[0][stage], axes[1][stage])
            parts = [sent[0]] + [shift_along(sent[d], now, d) for d in SHIFTS]
            if stage < 2:
                blocks[colour] = add_blocks(parts)
            else:
                last += parts

    first_slot = index_of({**here, CORE: 0}) * 4
    chip_orders = jnp.concatenate(
        [lax.dynamic_slice_in_dim(owner_table, first_slot + 8 * c, 4) for c in range(2)]
    )
    own, send, cross = finish(core_scalar, chip_orders, last)
    got = swap_cores(send)

    terms = jnp.transpose(cross.reshape(10, 64, 16), (1, 0, 2)).reshape(64, 160)
    nothing = jnp.zeros_like(terms)
    terms = jnp.concatenate([jnp.where(core == 0, terms, nothing), jnp.where(core == 1, terms, nothing)])
    power = lax.all_to_all(terms, BLK_GRP, 0, 0, tiled=True)
    power = jnp.sum(power, axis=0).reshape(10, 16)
    ells = my_index * 16 + lax.iota(jnp.int32, 16)
    spectra = power / (2 * ells + 1).astype(F32)[None, :]

    low, high = jnp.where(core == 0, own, got), jnp.where(core == 0, got, own)
    harmonics = jnp.concatenate([low, high], axis=-1).reshape(4, 4, 2, 2048)
    return harmonics, spectra


def solution(mesh):
    finer = Mesh(
        mesh.devices.reshape(4, 4, 2, 2, mesh.shape["grp"]),
        BLK_GRP,
    )
    in_specs = (P(None, BLK_GRP, None), P(BLK_GRP, None, None), P())
    out_specs = (P(BLK_GRP, None, None, None), P(None, BLK_GRP))
    return jax.shard_map(
        per_device, mesh=finer, in_specs=in_specs, out_specs=out_specs, check_vma=False
    )
```

```python
import functools
import math

import jax
import jax.numpy as jnp
import numpy as np
from jax import lax
from jax.experimental import pallas as pl
from jax.experimental.pallas import tpu as pltpu
from jax.sharding import Mesh
from jax.sharding import PartitionSpec as P

BLK_GRP = ("blk_0", "blk_1", "blk_2", "blk_3", "grp")
X, Y, Z, CORE = "blk_0", "blk_1", "z", "blk_3"
COLOURS = (
    (0, 768, ((X, Y, Z), (Y, Z, X))),
    (768, 256, ((Z, X, Y), (Z, X, Y))),
)
SHIFTS = (2, 1, 3)
F32, BF16 = jnp.float32, jnp.bfloat16
SMEM = pl.BlockSpec(memory_space=pltpu.SMEM)
VMEM = pl.BlockSpec(memory_space=pltpu.VMEM)
HBM = pl.BlockSpec(memory_space=pltpu.HBM)


def places(device):
    return {
        X: device // 32,
        Y: device // 8 % 4,
        Z: device % 2 * 2 + device // 4 % 2,
        CORE: device // 2 % 2,
    }


def index_of(place):
    z = place[Z]
    return place[X] * 32 + place[Y] * 8 + z % 2 * 4 + place[CORE] * 2 + z // 2


def shift_along(x, axes, shift):
    pairs = []
    for device in range(128):
        place = places(device)
        axis = axes[place[CORE]]
        pairs.append((device, index_of({**place, axis: (place[axis] + shift) % 4})))
    return lax.ppermute(x, BLK_GRP, pairs)


def swap_cores(x):
    return lax.ppermute(x, CORE, [(0, 1), (1, 0)])


def kernel_call(kernel, name, mib, flops, **kwargs):
    return pl.pallas_call(
        kernel,
        name=name,
        compiler_params=pltpu.CompilerParams(vmem_limit_bytes=mib << 20),
        cost_estimate=pl.CostEstimate(flops=flops, bytes_accessed=1 << 20, transcendentals=0),
        **kwargs,
    )


def half_copy(first, width, core_ref, leg_ref, out_ref, sem):
    start = pl.multiple_of((1 - core_ref[0]) * 1024 + first, 128)
    return pltpu.make_async_copy(leg_ref.at[:, :, pl.ds(start, width)], out_ref, sem)


def half_kernel(first, width, core_ref, leg_ref, out_ref, sem):
    copy = half_copy(first, width, core_ref, leg_ref, out_ref, sem)
    copy.start()
    copy.wait()


def other_half(first, width, core, legendre):
    return kernel_call(
        functools.partial(half_kernel, first, width),
        f"other_half_{first}",
        50,
        width * 8192,
        out_shape=jax.ShapeDtypeStruct((4, 512, width), BF16),
        in_specs=[SMEM, HBM],
        out_specs=VMEM,
        scratch_shapes=[pltpu.SemaphoreType.DMA],
    )(core, legendre)


def real_fft(values):
    n = len(values)
    if n == 1:
        return [(values[0], None)]
    even, odd = real_fft(values[0::2]), real_fft(values[1::2])
    half = n // 2
    out = []
    for k in range(half + 1):
        er, ei = pick(even, k % half, half)
        orr, oi = pick(odd, k % half, half)
        c, s = math.cos(2 * math.pi * k / n), math.sin(2 * math.pi * k / n)
        if k == 0:
            tr, ti = orr, oi
        elif 2 * k == n:
            tr, ti = -orr, (None if oi is None else -oi)
        elif 4 * k == n:
            tr, ti = oi, -orr
        else:
            tr = orr * c if oi is None else orr * c + oi * s
            ti = -orr * s if oi is None else oi * c - orr * s
        out.append((plus(er, tr), plus(ei, ti)))
    return out


def plus(a, b):
    if a is None:
        return b
    return a if b is None else a + b


def pick(spectrum, k, n):
    if k <= n // 2:
        return spectrum[k]
    re, im = spectrum[n - k]
    return re, (None if im is None else -im)


def fourier_kernel(
    first, width, core_ref, leg_ref, sky_ref, waves_ref, out_ref, half_ref, x_ref, cos_ref, sin_ref, tail_ref, z_ref, sems
):
    half = half_copy(first, width, core_ref, leg_ref, half_ref, sems.at[0])
    copies = [
        pltpu.make_async_copy(sky_ref, x_ref, sems.at[1]),
        pltpu.make_async_copy(waves_ref.at[0:32], cos_ref, sems.at[2]),
        pltpu.make_async_copy(waves_ref.at[32:64], sin_ref, sems.at[3]),
        pltpu.make_async_copy(waves_ref.at[64:320], tail_ref, sems.at[4]),
    ]
    for copy in copies:
        copy.start()
    half.start()
    for copy in copies:
        copy.wait()
    row = lax.broadcasted_iota(jnp.int32, (8, 128), 0)
    total = None
    for r in range(4):
        slabs = []
        for k in range(32):
            maps = [jnp.broadcast_to(x_ref[a, r : r + 1, 128 * k : 128 * k + 128], (8, 128)) for a in range(4)]
            low, high = jnp.where(row < 2, maps[0], maps[1]), jnp.where(row < 6, maps[2], maps[3])
            slabs.append(jnp.where(row < 4, low, high))
        spectrum = real_fft(slabs)
        for m in range(32):
            re, im = pick(spectrum, m, 32)
            c, s = cos_ref[m : m + 1, :], sin_ref[m : m + 1, :]
            if im is None:
                re, im = re * c, -re * s
            else:
                re, im = re * c + im * s, im * c - re * s
            z_ref[8 * m : 8 * m + 8, 0:128] = jnp.where(row % 2 == 0, re, im)
            z_ref[8 * m : 8 * m + 8, 128:256] = jnp.where(row % 2 == 0, im, -re)
        out = jnp.dot(z_ref[...], tail_ref[...], precision=lax.Precision.HIGHEST, preferred_element_type=F32)
        out = pltpu.roll(out, 16 * r, 1) if r else out
        total = out if total is None else total + out
    out_ref[...] = (total * (1.0 / 64.0)).astype(BF16)
    half.wait()


def fourier_and_half(first, width, core, legendre, sky_maps):
    turn = 2 * np.pi / 4096 * np.outer(np.arange(32), np.arange(128))
    last = 2 * np.pi / 128 * np.outer(np.arange(128), np.arange(16))
    tail = np.zeros((256, 128))
    tail[:128, :16] = np.cos(last)
    tail[128:, :16] = np.sin(last)
    waves = np.concatenate([np.cos(turn), np.sin(turn), tail])
    return kernel_call(
        functools.partial(fourier_kernel, first, width),
        "fourier_and_half",
        55,
        width * 8192,
        out_shape=[jax.ShapeDtypeStruct((256, 128), BF16), jax.ShapeDtypeStruct((4, 512, width), BF16)],
        in_specs=[SMEM] + [HBM] * 3,
        out_specs=[VMEM] * 2,
        scratch_shapes=[
            pltpu.VMEM((4, 4, 4096), F32),
            pltpu.VMEM((32, 128), F32),
            pltpu.VMEM((32, 128), F32),
            pltpu.VMEM((256, 128), F32),
            pltpu.VMEM((256, 256), F32),
            pltpu.SemaphoreType.DMA((5,)),
        ],
    )(core, legendre, sky_maps, jnp.asarray(waves, F32))


def order_weights(own_ref, got_ref, out_ref):
    columns = jnp.concatenate([own_ref[...], got_ref[...]], axis=1)
    k = lax.broadcasted_iota(jnp.int32, (256, 256), 0)
    n = lax.broadcasted_iota(jnp.int32, (256, 256), 1)
    cycle_of = jnp.where(k % 128 < 64, (k // 128) * 4 + (k % 128) // 16, -1)
    spread = jnp.where(cycle_of == n // 32, 1.0, 0.0).astype(BF16)
    keep = jnp.where((k // 8) == (n % 32), 1.0, 0.0).astype(BF16)
    for g in range(16):
        pick_group = jnp.where(n % 16 == g, 1.0, 0.0).astype(BF16)
        spread_out = jnp.dot(columns * pick_group, spread, preferred_element_type=F32)
        out_ref[g] = spread_out.astype(BF16) * keep


def slots_along(axis, me):
    out = []
    for d in range(4):
        at = (me + d) % 4
        out.append({X: at * 128, Y: at * 32, Z: at % 2 * 16 + at // 2 * 4}[axis])
    return out


def chip_sums_kernel(first, width, axes, here_ref, owner_ref, leg_ref, got_ref, own_f_ref, got_f_ref, *rest):
    outs, (table, weights, sums, sems) = rest[-8:-4], rest[-4:]
    core = here_ref[3]
    start = pl.multiple_of(core * 1024 + first, 128)
    copies = [
        pltpu.make_async_copy(
            leg_ref.at[:, 64 * g : 64 * g + 64, pl.ds(start, width)], table.at[:, 64 * g : 64 * g + 64, :], sems.at[g]
        )
        for g in range(8)
    ]
    for copy in copies:
        copy.start()
    order_weights(own_f_ref, got_f_ref, weights)
    for g in range(16):
        if g % 2 == 0:
            copies[g // 2].wait()
        rows = slice(32 * g, 32 * g + 32)
        values = jnp.concatenate([table[:, rows, :].reshape(128, width), got_ref[:, rows, :].reshape(128, width)])
        done = jnp.dot(weights[g], values, preferred_element_type=F32)
        sums[rows] = done.astype(BF16).reshape(32, 8, width)
    along = {axis: slots_along(axis, here_ref[k]) for k, axis in enumerate((X, Y, Z))}
    parts = []
    for on_0, on_1 in zip(*axes):
        if on_0 == on_1:
            parts.append(along[on_0])
        else:
            parts.append([jnp.where(core == 0, v0, v1) for v0, v1 in zip(along[on_0], along[on_1])])
    for a in range(4):
        for b in range(4):
            for c in range(4):
                chip = parts[0][a] + parts[1][b] + parts[2][c]
                for q in range(8):
                    slot = chip + q // 4 * 8 + q % 4
                    outs[a][(b * 4 + c) * 8 + q] = sums[owner_ref[slot]]


def chip_sums(first, width, axes, here, owner_table, legendre, got, own_f, got_f, *after):
    return kernel_call(
        functools.partial(chip_sums_kernel, first, width, axes),
        f"chip_sums_{first}",
        45,
        width * 1_000_000,
        out_shape=[jax.ShapeDtypeStruct((128, 8, width), BF16)] * 4,
        in_specs=[SMEM, SMEM, HBM, VMEM, VMEM, VMEM] + [HBM] * len(after),
        out_specs=[VMEM] * 4,
        scratch_shapes=[
            pltpu.VMEM((4, 512, width), BF16),
            pltpu.VMEM((16, 256, 256), BF16),
            pltpu.VMEM((512, 8, width), BF16),
            pltpu.SemaphoreType.DMA((8,)),
        ],
    )(here, owner_table, legendre, got, own_f, got_f, *after)


def add_kernel(own_ref, a_ref, b_ref, c_ref, *outs):
    count = outs[0].shape[0]
    for d, out in enumerate(outs):
        part = pl.ds(d * count, count)
        total = own_ref[part].astype(F32) + a_ref[part].astype(F32)
        total = total + b_ref[part].astype(F32) + c_ref[part].astype(F32)
        out[...] = total.astype(out.dtype)


def add_blocks(parts):
    count, rows, width = parts[0].shape
    return kernel_call(
        add_kernel,
        "add_blocks",
        12,
        count * width * 64,
        out_shape=[jax.ShapeDtypeStruct((count // 4, rows, width), F32 if d == 0 else BF16) for d in range(4)],
        in_specs=[VMEM] * 4,
        out_specs=[VMEM] * 4,
    )(*parts)


def finish_kernel(core_ref, order_ref, *refs):
    ins, (own_ref, send_ref, cross_ref) = refs[:-3], refs[-3:]
    core = core_ref[0]
    for colour, (first, width, _) in enumerate(COLOURS):
        lane = slice(first, first + width)
        ell = lax.broadcasted_iota(jnp.int32, (8, width), 1) + core * 1024 + first
        totals = [jnp.zeros((8, width), F32) for _ in range(4)]
        parts = ins[4 * colour : 4 * colour + 4]

        def slot_sum(slot):
            h = parts[0][slot].astype(F32) + parts[1][slot].astype(F32)
            h = h + parts[2][slot].astype(F32) + parts[3][slot].astype(F32)
            order = order_ref[slot]
            h = jnp.where(ell >= order, h, 0.0)
            weighted = h * jnp.where(order == 0, 1.0, 2.0)
            for delta in range(4):
                other = pltpu.roll(h, 8 - 2 * delta, 0) if delta else h
                totals[delta] = totals[delta] + weighted * other
            return h

        for j in range(4):
            own_ref[j, :, lane] = slot_sum(core * 4 + j)
            send_ref[j, :, lane] = slot_sum((1 - core) * 4 + j)
        row = 0
        for i in range(4):
            for j in range(i, 4):
                t = totals[j - i]
                cross_ref[row : row + 1, lane] = t[2 * i : 2 * i + 1] + t[2 * i + 1 : 2 * i + 2]
                row += 1


def finish(core, orders, parts):
    return kernel_call(
        finish_kernel,
        "finish",
        4,
        8 * 8 * 1024 * 16,
        out_shape=[
            jax.ShapeDtypeStruct((4, 8, 1024), F32),
            jax.ShapeDtypeStruct((4, 8, 1024), F32),
            jax.ShapeDtypeStruct((10, 1024), F32),
        ],
        in_specs=[SMEM, SMEM] + [VMEM] * len(parts),
        out_specs=[VMEM] * 3,
    )(core, orders, *parts)


def per_device(sky_maps, legendre, owner_table):
    my_index = lax.axis_index(BLK_GRP)
    here = places(my_index)
    core = here[CORE]
    core_scalar = core.reshape(1).astype(jnp.int32)

    here_scalars = jnp.stack([here[axis] for axis in (X, Y, Z, CORE)]).astype(jnp.int32)

    (first_a, width_a, axes_a), (first_b, width_b, axes_b) = COLOURS
    own_f, half_a = fourier_and_half(first_a, width_a, core_scalar, legendre, sky_maps)
    got_f, got_a = swap_cores(own_f), swap_cores(half_a)
    half_b = other_half(first_b, width_b, core_scalar, legendre)
    got_b = swap_cores(half_b)
    blocks = [
        chip_sums(first_a, width_a, axes_a, here_scalars, owner_table, legendre, got_a, own_f, got_f, half_b),
        chip_sums(first_b, width_b, axes_b, here_scalars, owner_table, legendre, got_b, own_f, got_f),
    ]
    last = []
    for stage in range(3):
        for colour, (_, _, axes) in enumerate(COLOURS):
            sent = blocks[colour]
            now = (axes[0][stage], axes[1][stage])
            parts = [sent[0]] + [shift_along(sent[d], now, d) for d in SHIFTS]
            if stage < 2:
                blocks[colour] = add_blocks(parts)
            else:
                last += parts

    first_slot = index_of({**here, CORE: 0}) * 4
    chip_orders = jnp.concatenate(
        [lax.dynamic_slice_in_dim(owner_table, first_slot + 8 * c, 4) for c in range(2)]
    )
    own, send, cross = finish(core_scalar, chip_orders, last)
    got = swap_cores(send)

    terms = jnp.transpose(cross.reshape(10, 64, 16), (1, 0, 2)).reshape(64, 160)
    nothing = jnp.zeros_like(terms)
    terms = jnp.concatenate([jnp.where(core == 0, terms, nothing), jnp.where(core == 1, terms, nothing)])
    power = lax.all_to_all(terms, BLK_GRP, 0, 0, tiled=True)
    power = jnp.sum(power, axis=0).reshape(10, 16)
    ells = my_index * 16 + lax.iota(jnp.int32, 16)
    spectra = power / (2 * ells + 1).astype(F32)[None, :]

    low, high = jnp.where(core == 0, own, got), jnp.where(core == 0, got, own)
    harmonics = jnp.concatenate([low, high], axis=-1).reshape(4, 4, 2, 2048)
    return harmonics, spectra


def solution(mesh):
    finer = Mesh(
        mesh.devices.reshape(4, 4, 2, 2, mesh.shape["grp"]),
        BLK_GRP,
    )
    in_specs = (P(None, BLK_GRP, None), P(BLK_GRP, None, None), P())
    out_specs = (P(BLK_GRP, None, None, None), P(None, BLK_GRP))
    return jax.shard_map(
        per_device, mesh=finer, in_specs=in_specs, out_specs=out_specs, check_vma=False
    )
```

```python
import functools
import math

import jax
import jax.numpy as jnp
import numpy as np
from jax import lax
from jax.experimental import pallas as pl
from jax.experimental.pallas import tpu as pltpu
from jax.sharding import Mesh
from jax.sharding import PartitionSpec as P


BLK_GRP = ("blk_0", "blk_1", "blk_2", "blk_3", "grp")
X, Y, Z, CORE = "blk_0", "blk_1", "z", "blk_3"
COLOURS = (
    (0, 768, ((X, Y, Z), (Y, Z, X))),
    (768, 256, ((Z, X, Y), (Z, X, Y))),
)
PIECES = ((0, 384, 0), (384, 384, 0), (768, 256, 1))
SHIFTS = (2, 1, 3)
F32, BF16 = jnp.float32, jnp.bfloat16
SMEM = pl.BlockSpec(memory_space=pltpu.SMEM)
VMEM = pl.BlockSpec(memory_space=pltpu.VMEM)
HBM = pl.BlockSpec(memory_space=pltpu.HBM)


def places(device):
    return {
        X: device // 32,
        Y: device // 8 % 4,
        Z: device % 2 * 2 + device // 4 % 2,
        CORE: device // 2 % 2,
    }


def index_of(place):
    z = place[Z]
    return place[X] * 32 + place[Y] * 8 + z % 2 * 4 + place[CORE] * 2 + z // 2


def shift_along(x, axes, shift):
    pairs = []
    for device in range(128):
        place = places(device)
        axis = axes[place[CORE]]
        pairs.append((device, index_of({**place, axis: (place[axis] + shift) % 4})))
    return lax.ppermute(x, BLK_GRP, pairs)


def swap_cores(x):
    return lax.ppermute(x, CORE, [(0, 1), (1, 0)])


def kernel_call(kernel, mib, flops, **kwargs):
    return pl.pallas_call(
        kernel,
        compiler_params=pltpu.CompilerParams(vmem_limit_bytes=mib << 20),
        cost_estimate=pl.CostEstimate(flops=flops, bytes_accessed=1 << 20, transcendentals=0),
        **kwargs,
    )


def half_copy(first, width, core_ref, leg_ref, out_ref, sem):
    start = pl.multiple_of((1 - core_ref[0]) * 1024 + first, 128)
    return pltpu.make_async_copy(leg_ref.at[:, :, pl.ds(start, width)], out_ref, sem)


def halves_kernel(core_ref, leg_ref, *rest):
    outs, sems = rest[:-1], rest[-1]
    copies = [
        half_copy(first, width, core_ref, leg_ref, out, sems.at[k])
        for k, ((first, width, _), out) in enumerate(zip(PIECES[1:], outs))
    ]
    for copy in copies:
        copy.start()
    for copy in copies:
        copy.wait()


def later_halves(core, legendre):
    return kernel_call(
        halves_kernel,
        48,
        1 << 20,
        out_shape=[jax.ShapeDtypeStruct((4, 512, width), BF16) for _, width, _ in PIECES[1:]],
        in_specs=[SMEM, HBM],
        out_specs=[VMEM] * len(PIECES[1:]),
        scratch_shapes=[pltpu.SemaphoreType.DMA((len(PIECES) - 1,))],
    )(core, legendre)


def real_fft(values):
    n = len(values)
    if n == 1:
        return [(values[0], None)]
    even, odd = real_fft(values[0::2]), real_fft(values[1::2])
    half = n // 2
    out = []
    for k in range(half + 1):
        er, ei = pick(even, k % half, half)
        orr, oi = pick(odd, k % half, half)
        c, s = math.cos(2 * math.pi * k / n), math.sin(2 * math.pi * k / n)
        if k == 0:
            tr, ti = orr, oi
        elif 2 * k == n:
            tr, ti = -orr, (None if oi is None else -oi)
        elif 4 * k == n:
            tr, ti = oi, -orr
        else:
            tr = orr * c if oi is None else orr * c + oi * s
            ti = -orr * s if oi is None else oi * c - orr * s
        out.append((plus(er, tr), plus(ei, ti)))
    return out


def plus(a, b):
    if a is None:
        return b
    return a if b is None else a + b


def pick(spectrum, k, n):
    if k <= n // 2:
        return spectrum[k]
    re, im = spectrum[n - k]
    return re, (None if im is None else -im)


def fourier_kernel(
    first, width, core_ref, leg_ref, sky_ref, waves_ref, out_ref, send_ref, half_ref, x_ref, cos_ref, sin_ref, tail_ref, z_ref, sems
):
    half = half_copy(first, width, core_ref, leg_ref, half_ref, sems.at[0])
    copies = [
        pltpu.make_async_copy(sky_ref, x_ref, sems.at[1]),
        pltpu.make_async_copy(waves_ref.at[0:32], cos_ref, sems.at[2]),
        pltpu.make_async_copy(waves_ref.at[32:64], sin_ref, sems.at[3]),
        pltpu.make_async_copy(waves_ref.at[64:320], tail_ref, sems.at[4]),
    ]
    for copy in copies:
        copy.start()
    half.start()
    for copy in copies:
        copy.wait()
    row = lax.broadcasted_iota(jnp.int32, (8, 128), 0)
    total = None
    for r in range(4):
        slabs = []
        for k in range(32):
            maps = [jnp.broadcast_to(x_ref[a, r : r + 1, 128 * k : 128 * k + 128], (8, 128)) for a in range(4)]
            low, high = jnp.where(row < 2, maps[0], maps[1]), jnp.where(row < 6, maps[2], maps[3])
            slabs.append(jnp.where(row < 4, low, high))
        spectrum = real_fft(slabs)
        for m in range(32):
            re, im = pick(spectrum, m, 32)
            c, s = cos_ref[m : m + 1, :], sin_ref[m : m + 1, :]
            if im is None:
                re, im = re * c, -re * s
            else:
                re, im = re * c + im * s, im * c - re * s
            z_ref[8 * m : 8 * m + 8, 0:128] = jnp.where(row % 2 == 0, re, im)
            z_ref[8 * m : 8 * m + 8, 128:256] = jnp.where(row % 2 == 0, im, -re)
        out = jnp.dot(z_ref[...], tail_ref[...], precision=lax.Precision.HIGHEST, preferred_element_type=F32)
        out = pltpu.roll(out, 16 * r, 1) if r else out
        total = out if total is None else total + out
    rounded = (total * (1.0 / 64.0)).astype(BF16)
    out_ref[...] = rounded
    send_ref[...] = rounded
    half.wait()


def fourier_and_half(first, width, core, legendre, sky_maps):
    turn = 2 * np.pi / 4096 * np.outer(np.arange(32), np.arange(128))
    last = 2 * np.pi / 128 * np.outer(np.arange(128), np.arange(16))
    tail = np.zeros((256, 128))
    tail[:128, :16] = np.cos(last)
    tail[128:, :16] = np.sin(last)
    waves = np.concatenate([np.cos(turn), np.sin(turn), tail])
    return kernel_call(
        functools.partial(fourier_kernel, first, width),
        55,
        width * 8192,
        out_shape=[jax.ShapeDtypeStruct((256, 128), BF16)] * 2 + [jax.ShapeDtypeStruct((4, 512, width), BF16)],
        in_specs=[SMEM] + [HBM] * 3,
        out_specs=[VMEM] * 3,
        scratch_shapes=[
            pltpu.VMEM((4, 4, 4096), F32),
            pltpu.VMEM((32, 128), F32),
            pltpu.VMEM((32, 128), F32),
            pltpu.VMEM((256, 128), F32),
            pltpu.VMEM((256, 256), F32),
            pltpu.SemaphoreType.DMA((5,)),
        ],
    )(core, legendre, sky_maps, jnp.asarray(waves, F32))


def weights_kernel(core_ref, leg_ref, own_ref, got_ref, *rest):
    out_ref, table_ref, sem = rest[-3:]
    start = pl.multiple_of(core_ref[0] * 1024, 128)
    copy = pltpu.make_async_copy(leg_ref.at[:, :, pl.ds(start, 1024)], table_ref, sem)
    copy.start()
    order_weights(own_ref, got_ref, out_ref)
    copy.wait()


def weights_and_own_half(core, legendre, own_f, got_f, *after):
    return kernel_call(
        weights_kernel,
        42,
        1 << 26,
        out_shape=[jax.ShapeDtypeStruct((16, 256, 256), BF16), jax.ShapeDtypeStruct((4, 512, 1024), BF16)],
        in_specs=[SMEM, HBM, VMEM, VMEM] + [HBM] * len(after),
        out_specs=[VMEM] * 2,
        scratch_shapes=[pltpu.SemaphoreType.DMA],
    )(core, legendre, own_f, got_f, *after)


def order_weights(own_ref, got_ref, out_ref):
    columns = jnp.concatenate([own_ref[...], got_ref[...]], axis=1)
    k = lax.broadcasted_iota(jnp.int32, (256, 256), 0)
    n = lax.broadcasted_iota(jnp.int32, (256, 256), 1)
    cycle_of = jnp.where(k % 128 < 64, (k // 128) * 4 + (k % 128) // 16, -1)
    spread = jnp.where(cycle_of == n // 32, 1.0, 0.0).astype(BF16)
    keep = jnp.where((k // 8) == (n % 32), 1.0, 0.0).astype(BF16)
    for g in range(16):
        pick_group = jnp.where(n % 16 == g, 1.0, 0.0).astype(BF16)
        spread_out = jnp.dot(columns * pick_group, spread, preferred_element_type=F32)
        out_ref[g] = spread_out.astype(BF16) * keep


def slots_along(axis, me):
    out = []
    for d in range(4):
        at = (me + d) % 4
        out.append({X: at * 128, Y: at * 32, Z: at % 2 * 16 + at // 2 * 4}[axis])
    return out


def chip_sums_kernel(first, width, axes, here_ref, owner_ref, weights, table, got_ref, *rest):
    outs, sums = rest[-5:-1], rest[-1]
    core = here_ref[3]
    for g in range(16):
        rows = slice(32 * g, 32 * g + 32)
        own = table[:, rows, first : first + width].reshape(128, width)
        values = jnp.concatenate([own, got_ref[:, rows, :].reshape(128, width)])
        done = jnp.dot(weights[g], values, preferred_element_type=F32)
        sums[rows] = done.astype(BF16).reshape(32, 8, width)
    along = {axis: slots_along(axis, here_ref[k]) for k, axis in enumerate((X, Y, Z))}
    parts = []
    for on_0, on_1 in zip(*axes):
        if on_0 == on_1:
            parts.append(along[on_0])
        else:
            parts.append([jnp.where(core == 0, v0, v1) for v0, v1 in zip(along[on_0], along[on_1])])
    for a in range(4):
        for b in range(4):
            for c in range(4):
                chip = parts[0][a] + parts[1][b] + parts[2][c]
                for q in range(8):
                    slot = chip + q // 4 * 8 + q % 4
                    outs[a][(b * 4 + c) * 8 + q] = sums[owner_ref[slot]]


def chip_sums(piece, here, owner_table, weights, table, got, *after):
    first, width, colour = piece
    return kernel_call(
        functools.partial(chip_sums_kernel, first, width, COLOURS[colour][2]),
        20,
        width * 1_000_000,
        out_shape=[jax.ShapeDtypeStruct((128, 8, width), BF16)] * 4,
        in_specs=[SMEM, SMEM, VMEM, VMEM, VMEM] + [HBM] * len(after),
        out_specs=[VMEM] * 4,
        scratch_shapes=[pltpu.VMEM((512, 8, width), BF16)],
    )(here, owner_table, weights, table, got, *after)


def add_kernel(pieces, *refs):
    ins, outs = refs[: 4 * pieces], refs[-4:]
    count = outs[0].shape[0]
    for d, out in enumerate(outs):
        part = pl.ds(d * count, count)
        lane = 0
        for k in range(pieces):
            own, a, b, c = ins[4 * k : 4 * k + 4]
            total = own[part].astype(F32) + a[part].astype(F32)
            total = total + b[part].astype(F32) + c[part].astype(F32)
            out[:, :, lane : lane + own.shape[2]] = total.astype(out.dtype)
            lane += own.shape[2]


def add_blocks(pieces, *after):
    count, rows, _ = pieces[0][0].shape
    width = sum(parts[0].shape[2] for parts in pieces)
    return kernel_call(
        functools.partial(add_kernel, len(pieces)),
        12,
        count * width * 64,
        out_shape=[jax.ShapeDtypeStruct((count // 4, rows, width), F32 if d == 0 else BF16) for d in range(4)],
        in_specs=[VMEM] * (4 * len(pieces)) + [HBM] * len(after),
        out_specs=[VMEM] * 4,
    )(*[block for parts in pieces for block in parts], *after)


def finish_kernel(core_ref, order_ref, *refs):
    ins, (own_ref, send_ref, cross_ref) = refs[:-3], refs[-3:]
    core = core_ref[0]
    for colour, (first, width, _) in enumerate(COLOURS):
        lane = slice(first, first + width)
        ell = lax.broadcasted_iota(jnp.int32, (8, width), 1) + core * 1024 + first
        totals = [jnp.zeros((8, width), F32) for _ in range(4)]
        parts = ins[4 * colour : 4 * colour + 4]

        def slot_sum(slot):
            h = parts[0][slot].astype(F32) + parts[1][slot].astype(F32)
            h = h + parts[2][slot].astype(F32) + parts[3][slot].astype(F32)
            order = order_ref[slot]
            h = jnp.where(ell >= order, h, 0.0)
            weighted = h * jnp.where(order == 0, 1.0, 2.0)
            for delta in range(4):
                other = pltpu.roll(h, 8 - 2 * delta, 0) if delta else h
                totals[delta] = totals[delta] + weighted * other
            return h

        for j in range(4):
            own_ref[j, :, lane] = slot_sum(core * 4 + j)
            send_ref[j, :, lane] = slot_sum((1 - core) * 4 + j)
        row = 0
        for i in range(4):
            for j in range(i, 4):
                t = totals[j - i]
                cross_ref[row : row + 1, lane] = t[2 * i : 2 * i + 1] + t[2 * i + 1 : 2 * i + 2]
                row += 1


def finish(core, orders, parts):
    return kernel_call(
        finish_kernel,
        4,
        8 * 8 * 1024 * 16,
        out_shape=[
            jax.ShapeDtypeStruct((4, 8, 1024), F32),
            jax.ShapeDtypeStruct((4, 8, 1024), F32),
            jax.ShapeDtypeStruct((10, 1024), F32),
        ],
        in_specs=[SMEM, SMEM] + [VMEM] * len(parts),
        out_specs=[VMEM] * 3,
    )(core, orders, *parts)


def steps(sky_maps, legendre, owner_table):
    my_index = lax.axis_index(BLK_GRP)
    here = places(my_index)
    core = here[CORE]
    core_scalar = core.reshape(1).astype(jnp.int32)

    here_scalars = jnp.stack([here[axis] for axis in (X, Y, Z, CORE)]).astype(jnp.int32)

    own_f, send_f, half = fourier_and_half(*PIECES[0][:2], core_scalar, legendre, sky_maps)
    got_f = swap_cores(send_f)
    received = [swap_cores(half)]
    halves = later_halves(core_scalar, legendre)
    received += [swap_cores(half) for half in halves]
    weights, table = weights_and_own_half(core_scalar, legendre, own_f, got_f, *halves)

    def exchange(sent, stage, colour):
        axes = COLOURS[colour][2]
        now = (axes[0][stage], axes[1][stage])
        return [sent[0]] + [shift_along(sent[d], now, d) for d in SHIFTS]

    pieces = [[], []]
    after = []
    for piece, got in zip(PIECES, received):
        sent = chip_sums(piece, here_scalars, owner_table, weights, table, got, *after)
        pieces[piece[2]].append(exchange(sent, 0, piece[2]))
        after = sent[:1]
    last, after = [], []
    for stage in (1, 2):
        for colour in range(2):
            sent = add_blocks(pieces[colour], *after)
            after = sent[:1]
            pieces[colour] = [exchange(sent, stage, colour)]
    last = pieces[0][0] + pieces[1][0]

    first_slot = index_of({**here, CORE: 0}) * 4
    chip_orders = jnp.concatenate(
        [lax.dynamic_slice_in_dim(owner_table, first_slot + 8 * c, 4) for c in range(2)]
    )
    own, send, cross = finish(core_scalar, chip_orders, last)
    got = swap_cores(send)

    terms = jnp.transpose(cross.reshape(10, 64, 16), (1, 0, 2)).reshape(64, 160)
    nothing = jnp.zeros_like(terms)
    terms = jnp.concatenate([jnp.where(core == 0, terms, nothing), jnp.where(core == 1, terms, nothing)])
    power = lax.all_to_all(terms, BLK_GRP, 0, 0, tiled=True)
    power = jnp.sum(power, axis=0).reshape(10, 16)
    ells = my_index * 16 + lax.iota(jnp.int32, 16)
    spectra = power / (2 * ells + 1).astype(F32)[None, :]

    low, high = jnp.where(core == 0, own, got), jnp.where(core == 0, got, own)
    harmonics = jnp.concatenate([low, high], axis=-1).reshape(4, 4, 2, 2048)
    return harmonics, spectra


def solution(mesh):
    finer = Mesh(
        mesh.devices.reshape(4, 4, 2, 2, mesh.shape["grp"]),
        BLK_GRP,
    )
    in_specs = (P(None, BLK_GRP, None), P(BLK_GRP, None, None), P())
    out_specs = (P(BLK_GRP, None, None, None), P(None, BLK_GRP))
    return jax.shard_map(steps, mesh=finer, in_specs=in_specs, out_specs=out_specs, check_vma=False)
```

```python
import functools
import math

import jax
import jax.numpy as jnp
import numpy as np
from jax import lax
from jax.experimental import pallas as pl
from jax.experimental.pallas import tpu as pltpu
from jax.sharding import Mesh
from jax.sharding import PartitionSpec as P


BLK_GRP = ("blk_0", "blk_1", "blk_2", "blk_3", "grp")
X, Y, Z, CORE = "blk_0", "blk_1", "z", "blk_3"
COLOURS = (
    (0, 768, ((X, Y, Z), (Y, Z, X))),
    (768, 256, ((Z, X, Y), (Z, X, Y))),
)
PIECES = ((0, 512, 0), (512, 256, 0), (768, 256, 1))
SHIFTS = (2, 1, 3)
F32, BF16 = jnp.float32, jnp.bfloat16
SMEM = pl.BlockSpec(memory_space=pltpu.SMEM)
VMEM = pl.BlockSpec(memory_space=pltpu.VMEM)
HBM = pl.BlockSpec(memory_space=pltpu.HBM)


def places(device):
    return {
        X: device // 32,
        Y: device // 8 % 4,
        Z: device % 2 * 2 + device // 4 % 2,
        CORE: device // 2 % 2,
    }


def index_of(place):
    z = place[Z]
    return place[X] * 32 + place[Y] * 8 + z % 2 * 4 + place[CORE] * 2 + z // 2


def shift_along(x, axes, shift):
    pairs = []
    for device in range(128):
        place = places(device)
        axis = axes[place[CORE]]
        pairs.append((device, index_of({**place, axis: (place[axis] + shift) % 4})))
    return lax.ppermute(x, BLK_GRP, pairs)


def swap_cores(x):
    return lax.ppermute(x, CORE, [(0, 1), (1, 0)])


def kernel_call(kernel, mib, flops, **kwargs):
    return pl.pallas_call(
        kernel,
        compiler_params=pltpu.CompilerParams(vmem_limit_bytes=mib << 20),
        cost_estimate=pl.CostEstimate(flops=flops, bytes_accessed=1 << 20, transcendentals=0),
        **kwargs,
    )


def half_copy(first, width, core_ref, leg_ref, out_ref, sem):
    start = pl.multiple_of((1 - core_ref[0]) * 1024 + first, 128)
    return pltpu.make_async_copy(leg_ref.at[:, :, pl.ds(start, width)], out_ref, sem)


def halves_kernel(core_ref, leg_ref, *rest):
    outs, sems = rest[:-1], rest[-1]
    copies = [
        half_copy(first, width, core_ref, leg_ref, out, sems.at[k])
        for k, ((first, width, _), out) in enumerate(zip(PIECES[1:], outs))
    ]
    for copy in copies:
        copy.start()
    for copy in copies:
        copy.wait()


def later_halves(core, legendre):
    return kernel_call(
        halves_kernel,
        48,
        1 << 20,
        out_shape=[jax.ShapeDtypeStruct((4, 512, width), BF16) for _, width, _ in PIECES[1:]],
        in_specs=[SMEM, HBM],
        out_specs=[VMEM] * len(PIECES[1:]),
        scratch_shapes=[pltpu.SemaphoreType.DMA((len(PIECES) - 1,))],
    )(core, legendre)


def real_fft(values):
    n = len(values)
    if n == 1:
        return [(values[0], None)]
    even, odd = real_fft(values[0::2]), real_fft(values[1::2])
    half = n // 2
    out = []
    for k in range(half + 1):
        er, ei = pick(even, k % half, half)
        orr, oi = pick(odd, k % half, half)
        c, s = math.cos(2 * math.pi * k / n), math.sin(2 * math.pi * k / n)
        if k == 0:
            tr, ti = orr, oi
        elif 2 * k == n:
            tr, ti = -orr, (None if oi is None else -oi)
        elif 4 * k == n:
            tr, ti = oi, -orr
        else:
            tr = orr * c if oi is None else orr * c + oi * s
            ti = -orr * s if oi is None else oi * c - orr * s
        out.append((plus(er, tr), plus(ei, ti)))
    return out


def plus(a, b):
    if a is None:
        return b
    return a if b is None else a + b


def pick(spectrum, k, n):
    if k <= n // 2:
        return spectrum[k]
    re, im = spectrum[n - k]
    return re, (None if im is None else -im)


def fourier_kernel(
    first, width, core_ref, leg_ref, sky_ref, waves_ref, out_ref, send_ref, half_ref, x_ref, cos_ref, sin_ref, tail_ref, z_ref, sems
):
    half = half_copy(first, width, core_ref, leg_ref, half_ref, sems.at[0])
    copies = [
        pltpu.make_async_copy(sky_ref, x_ref, sems.at[1]),
        pltpu.make_async_copy(waves_ref.at[0:32], cos_ref, sems.at[2]),
        pltpu.make_async_copy(waves_ref.at[32:64], sin_ref, sems.at[3]),
        pltpu.make_async_copy(waves_ref.at[64:320], tail_ref, sems.at[4]),
    ]
    for copy in copies:
        copy.start()
    half.start()
    for copy in copies:
        copy.wait()
    row = lax.broadcasted_iota(jnp.int32, (8, 128), 0)
    total = None
    for r in range(4):
        slabs = []
        for k in range(32):
            maps = [jnp.broadcast_to(x_ref[a, r : r + 1, 128 * k : 128 * k + 128], (8, 128)) for a in range(4)]
            low, high = jnp.where(row < 2, maps[0], maps[1]), jnp.where(row < 6, maps[2], maps[3])
            slabs.append(jnp.where(row < 4, low, high))
        spectrum = real_fft(slabs)
        for m in range(32):
            re, im = pick(spectrum, m, 32)
            c, s = cos_ref[m : m + 1, :], sin_ref[m : m + 1, :]
            if im is None:
                re, im = re * c, -re * s
            else:
                re, im = re * c + im * s, im * c - re * s
            z_ref[8 * m : 8 * m + 8, 0:128] = jnp.where(row % 2 == 0, re, im)
            z_ref[8 * m : 8 * m + 8, 128:256] = jnp.where(row % 2 == 0, im, -re)
        out = jnp.dot(z_ref[...], tail_ref[...], precision=lax.Precision.HIGHEST, preferred_element_type=F32)
        out = pltpu.roll(out, 16 * r, 1) if r else out
        total = out if total is None else total + out
    rounded = (total * (1.0 / 64.0)).astype(BF16)
    out_ref[...] = rounded
    send_ref[...] = rounded
    half.wait()


def fourier_and_half(first, width, core, legendre, sky_maps):
    turn = 2 * np.pi / 4096 * np.outer(np.arange(32), np.arange(128))
    last = 2 * np.pi / 128 * np.outer(np.arange(128), np.arange(16))
    tail = np.zeros((256, 128))
    tail[:128, :16] = np.cos(last)
    tail[128:, :16] = np.sin(last)
    waves = np.concatenate([np.cos(turn), np.sin(turn), tail])
    return kernel_call(
        functools.partial(fourier_kernel, first, width),
        55,
        width * 8192,
        out_shape=[jax.ShapeDtypeStruct((256, 128), BF16)] * 2 + [jax.ShapeDtypeStruct((4, 512, width), BF16)],
        in_specs=[SMEM] + [HBM] * 3,
        out_specs=[VMEM] * 3,
        scratch_shapes=[
            pltpu.VMEM((4, 4, 4096), F32),
            pltpu.VMEM((32, 128), F32),
            pltpu.VMEM((32, 128), F32),
            pltpu.VMEM((256, 128), F32),
            pltpu.VMEM((256, 256), F32),
            pltpu.SemaphoreType.DMA((5,)),
        ],
    )(core, legendre, sky_maps, jnp.asarray(waves, F32))


def weights_kernel(core_ref, leg_ref, own_ref, got_ref, *rest):
    out_ref, table_ref, sem = rest[-3:]
    start = pl.multiple_of(core_ref[0] * 1024, 128)
    copy = pltpu.make_async_copy(leg_ref.at[:, :, pl.ds(start, 1024)], table_ref, sem)
    copy.start()
    order_weights(own_ref, got_ref, out_ref)
    copy.wait()


def weights_and_own_half(core, legendre, own_f, got_f, *after):
    return kernel_call(
        weights_kernel,
        42,
        1 << 26,
        out_shape=[jax.ShapeDtypeStruct((16, 256, 256), BF16), jax.ShapeDtypeStruct((4, 512, 1024), BF16)],
        in_specs=[SMEM, HBM, VMEM, VMEM] + [HBM] * len(after),
        out_specs=[VMEM] * 2,
        scratch_shapes=[pltpu.SemaphoreType.DMA],
    )(core, legendre, own_f, got_f, *after)


def order_weights(own_ref, got_ref, out_ref):
    columns = jnp.concatenate([own_ref[...], got_ref[...]], axis=1)
    k = lax.broadcasted_iota(jnp.int32, (256, 256), 0)
    n = lax.broadcasted_iota(jnp.int32, (256, 256), 1)
    cycle_of = jnp.where(k % 128 < 64, (k // 128) * 4 + (k % 128) // 16, -1)
    spread = jnp.where(cycle_of == n // 32, 1.0, 0.0).astype(BF16)
    keep = jnp.where((k // 8) == (n % 32), 1.0, 0.0).astype(BF16)
    for g in range(16):
        pick_group = jnp.where(n % 16 == g, 1.0, 0.0).astype(BF16)
        spread_out = jnp.dot(columns * pick_group, spread, preferred_element_type=F32)
        out_ref[g] = spread_out.astype(BF16) * keep


def slots_along(axis, me):
    out = []
    for d in range(4):
        at = (me + d) % 4
        out.append({X: at * 128, Y: at * 32, Z: at % 2 * 16 + at // 2 * 4}[axis])
    return out


def chip_sums_kernel(first, width, axes, here_ref, owner_ref, weights, table, got_ref, *rest):
    outs, sums = rest[-5:-1], rest[-1]
    core = here_ref[3]
    for g in range(16):
        rows = slice(32 * g, 32 * g + 32)
        own = table[:, rows, first : first + width].reshape(128, width)
        values = jnp.concatenate([own, got_ref[:, rows, :].reshape(128, width)])
        done = jnp.dot(weights[g], values, preferred_element_type=F32)
        sums[rows] = done.astype(BF16).reshape(32, 8, width)
    along = {axis: slots_along(axis, here_ref[k]) for k, axis in enumerate((X, Y, Z))}
    parts = []
    for on_0, on_1 in zip(*axes):
        if on_0 == on_1:
            parts.append(along[on_0])
        else:
            parts.append([jnp.where(core == 0, v0, v1) for v0, v1 in zip(along[on_0], along[on_1])])
    for a in range(4):
        for b in range(4):
            for c in range(4):
                chip = parts[0][a] + parts[1][b] + parts[2][c]
                for q in range(8):
                    slot = chip + q // 4 * 8 + q % 4
                    outs[a][(b * 4 + c) * 8 + q] = sums[owner_ref[slot]]


def chip_sums(piece, here, owner_table, weights, table, got, *after):
    first, width, colour = piece
    return kernel_call(
        functools.partial(chip_sums_kernel, first, width, COLOURS[colour][2]),
        20,
        width * 1_000_000,
        out_shape=[jax.ShapeDtypeStruct((128, 8, width), BF16)] * 4,
        in_specs=[SMEM, SMEM, VMEM, VMEM, VMEM] + [HBM] * len(after),
        out_specs=[VMEM] * 4,
        scratch_shapes=[pltpu.VMEM((512, 8, width), BF16)],
    )(here, owner_table, weights, table, got, *after)


def total_of(refs, part):
    total = refs[0][part].astype(F32)
    for ref in refs[1:]:
        total = total + ref[part].astype(F32)
    return total


def add_kernel(counts, *refs):
    outs = refs[-4:]
    count = outs[0].shape[0]
    for d, out in enumerate(outs):
        part = pl.ds(d * count, count)
        lane, k = 0, 0
        for n in counts:
            total = total_of(refs[k : k + n], part)
            out[:, :, lane : lane + total.shape[2]] = total.astype(out.dtype)
            lane, k = lane + total.shape[2], k + n


def add_blocks(pieces, *after):
    count, rows, _ = pieces[0][0].shape
    width = sum(parts[0].shape[2] for parts in pieces)
    counts = [len(parts) for parts in pieces]
    return kernel_call(
        functools.partial(add_kernel, counts),
        12,
        count * width * 64,
        out_shape=[jax.ShapeDtypeStruct((count // 4, rows, width), F32 if d == 0 else BF16) for d in range(4)],
        in_specs=[VMEM] * sum(counts) + [HBM] * len(after),
        out_specs=[VMEM] * 4,
    )(*[block for parts in pieces for block in parts], *after)


def combine_kernel(a_ref, b_ref, *rest):
    everything = pl.ds(0, a_ref.shape[0])
    rest[-1][...] = total_of((a_ref, b_ref), everything).astype(BF16)


def combine(a, b, *after):
    return kernel_call(
        combine_kernel,
        8,
        a.size,
        out_shape=jax.ShapeDtypeStruct(a.shape, BF16),
        in_specs=[VMEM] * 2 + [HBM] * len(after),
        out_specs=VMEM,
    )(a, b, *after)


def finish_kernel(core_ref, order_ref, *refs):
    ins, (own_ref, send_ref, cross_ref) = refs[:-3], refs[-3:]
    core = core_ref[0]
    for colour, (first, width, _) in enumerate(COLOURS):
        lane = slice(first, first + width)
        ell = lax.broadcasted_iota(jnp.int32, (8, width), 1) + core * 1024 + first
        totals = [jnp.zeros((8, width), F32) for _ in range(4)]
        parts = ins[4 * colour : 4 * colour + 4]

        def slot_sum(slot):
            h = parts[0][slot].astype(F32) + parts[1][slot].astype(F32)
            h = h + parts[2][slot].astype(F32) + parts[3][slot].astype(F32)
            order = order_ref[slot]
            h = jnp.where(ell >= order, h, 0.0)
            weighted = h * jnp.where(order == 0, 1.0, 2.0)
            for delta in range(4):
                other = pltpu.roll(h, 8 - 2 * delta, 0) if delta else h
                totals[delta] = totals[delta] + weighted * other
            return h

        for j in range(4):
            own_ref[j, :, lane] = slot_sum(core * 4 + j)
            send_ref[j, :, lane] = slot_sum((1 - core) * 4 + j)
        row = 0
        for i in range(4):
            for j in range(i, 4):
                t = totals[j - i]
                cross_ref[row : row + 1, lane] = t[2 * i : 2 * i + 1] + t[2 * i + 1 : 2 * i + 2]
                row += 1


def finish(core, orders, parts):
    return kernel_call(
        finish_kernel,
        4,
        8 * 8 * 1024 * 16,
        out_shape=[
            jax.ShapeDtypeStruct((4, 8, 1024), F32),
            jax.ShapeDtypeStruct((4, 8, 1024), F32),
            jax.ShapeDtypeStruct((10, 1024), F32),
        ],
        in_specs=[SMEM, SMEM] + [VMEM] * len(parts),
        out_specs=[VMEM] * 3,
    )(core, orders, *parts)


def steps(sky_maps, legendre, owner_table):
    my_index = lax.axis_index(BLK_GRP)
    here = places(my_index)
    core = here[CORE]
    core_scalar = core.reshape(1).astype(jnp.int32)

    here_scalars = jnp.stack([here[axis] for axis in (X, Y, Z, CORE)]).astype(jnp.int32)

    own_f, send_f, half = fourier_and_half(*PIECES[0][:2], core_scalar, legendre, sky_maps)
    got_f = swap_cores(send_f)
    got_0 = swap_cores(half)
    half_1, half_2 = later_halves(core_scalar, legendre)
    got_1, got_2 = swap_cores(half_1), swap_cores(half_2)
    weights, table = weights_and_own_half(core_scalar, legendre, own_f, got_f, half_1, half_2)

    def move(block, stage, colour, shift):
        axes = COLOURS[colour][2]
        return shift_along(block, (axes[0][stage], axes[1][stage]), shift)

    def exchange(sent, stage, colour):
        return [sent[0]] + [move(sent[d], stage, colour, d) for d in SHIFTS]

    def sums_of(k, got, *after):
        return chip_sums(PIECES[k], here_scalars, owner_table, weights, table, got, *after)

    up = sums_of(0, got_0)
    through_up, from_above = move(up[2], 0, 0, 1), move(up[3], 0, 0, 3)
    down = sums_of(1, got_1)
    through_down, from_below = move(down[2], 0, 0, 3), move(down[1], 0, 0, 1)
    sent = sums_of(2, got_2, down[0])
    colour_1 = [exchange(sent, 0, 1)]
    both_up = combine(up[1], through_up, sent[0])
    from_below_up = move(both_up, 0, 0, 1)
    both_down = combine(down[3], through_down, both_up)
    from_above_down = move(both_down, 0, 0, 3)
    colour_0 = [[up[0], from_above, from_below_up], [down[0], from_below, from_above_down]]
    pieces = [colour_0, colour_1]
    after = []
    for stage in (1, 2):
        for colour in (0, 1):
            sent = add_blocks(pieces[colour], *after)
            after = sent[:1]
            pieces[colour] = [exchange(sent, stage, colour)]
    last = pieces[0][0] + pieces[1][0]

    first_slot = index_of({**here, CORE: 0}) * 4
    chip_orders = jnp.concatenate(
        [lax.dynamic_slice_in_dim(owner_table, first_slot + 8 * c, 4) for c in range(2)]
    )
    own, send, cross = finish(core_scalar, chip_orders, last)
    got = swap_cores(send)

    terms = jnp.transpose(cross.reshape(10, 64, 16), (1, 0, 2)).reshape(64, 160)
    nothing = jnp.zeros_like(terms)
    terms = jnp.concatenate([jnp.where(core == 0, terms, nothing), jnp.where(core == 1, terms, nothing)])
    power = lax.all_to_all(terms, BLK_GRP, 0, 0, tiled=True)
    power = jnp.sum(power, axis=0).reshape(10, 16)
    ells = my_index * 16 + lax.iota(jnp.int32, 16)
    spectra = power / (2 * ells + 1).astype(F32)[None, :]

    low, high = jnp.where(core == 0, own, got), jnp.where(core == 0, got, own)
    harmonics = jnp.concatenate([low, high], axis=-1)
    harmonics = harmonics.reshape(4, 4, 2, 2048)
    return harmonics, spectra


def solution(mesh):
    finer = Mesh(
        mesh.devices.reshape(4, 4, 2, 2, mesh.shape["grp"]),
        BLK_GRP,
    )
    in_specs = (P(None, BLK_GRP, None), P(BLK_GRP, None, None), P())
    out_specs = (P(BLK_GRP, None, None, None), P(None, BLK_GRP))
    return jax.shard_map(steps, mesh=finer, in_specs=in_specs, out_specs=out_specs, check_vma=False)
```

```python
import functools
import math

import jax
import jax.numpy as jnp
import numpy as np
from jax import lax
from jax.experimental import pallas as pl
from jax.experimental.pallas import tpu as pltpu
from jax.sharding import Mesh
from jax.sharding import PartitionSpec as P


BLK_GRP = ("blk_0", "blk_1", "blk_2", "blk_3", "grp")
X, Y, Z, CORE = "blk_0", "blk_1", "z", "blk_3"
COLOURS = (
    (0, 768, ((X, Y, Z), (Y, Z, X))),
    (768, 256, ((Z, X, Y), (Z, X, Y))),
)
PIECES = ((0, 512, 0), (512, 256, 0), (768, 256, 1))
SHIFTS = (2, 1, 3)
F32, BF16 = jnp.float32, jnp.bfloat16
SMEM = pl.BlockSpec(memory_space=pltpu.SMEM)
VMEM = pl.BlockSpec(memory_space=pltpu.VMEM)
HBM = pl.BlockSpec(memory_space=pltpu.HBM)


def places(device):
    return {
        X: device // 32,
        Y: device // 8 % 4,
        Z: device % 2 * 2 + device // 4 % 2,
        CORE: device // 2 % 2,
    }


def index_of(place):
    z = place[Z]
    return place[X] * 32 + place[Y] * 8 + z % 2 * 4 + place[CORE] * 2 + z // 2


def shift_along(x, axes, shift):
    pairs = []
    for device in range(128):
        place = places(device)
        axis = axes[place[CORE]]
        pairs.append((device, index_of({**place, axis: (place[axis] + shift) % 4})))
    return lax.ppermute(x, BLK_GRP, pairs)


def swap_cores(x):
    return lax.ppermute(x, CORE, [(0, 1), (1, 0)])


def kernel_call(kernel, mib, flops, **kwargs):
    return pl.pallas_call(
        kernel,
        compiler_params=pltpu.CompilerParams(vmem_limit_bytes=mib << 20),
        cost_estimate=pl.CostEstimate(flops=flops, bytes_accessed=1 << 20, transcendentals=0),
        **kwargs,
    )


def half_copy(first, width, core_ref, leg_ref, out_ref, sem):
    start = pl.multiple_of((1 - core_ref[0]) * 1024 + first, 128)
    return pltpu.make_async_copy(leg_ref.at[:, :, pl.ds(start, width)], out_ref, sem)


def half_kernel(core_ref, leg_ref, out_ref, sem):
    copy = half_copy(*PIECES[1][:2], core_ref, leg_ref, out_ref, sem)
    copy.start()
    copy.wait()


def second_half(core, legendre):
    return kernel_call(
        half_kernel,
        50,
        1 << 20,
        out_shape=jax.ShapeDtypeStruct((4, 512, PIECES[1][1]), BF16),
        in_specs=[SMEM, HBM],
        out_specs=VMEM,
        scratch_shapes=[pltpu.SemaphoreType.DMA],
    )(core, legendre)


def real_fft(values):
    n = len(values)
    if n == 1:
        return [(values[0], None)]
    even, odd = real_fft(values[0::2]), real_fft(values[1::2])
    half = n // 2
    out = []
    for k in range(half + 1):
        er, ei = pick(even, k % half, half)
        orr, oi = pick(odd, k % half, half)
        c, s = math.cos(2 * math.pi * k / n), math.sin(2 * math.pi * k / n)
        if k == 0:
            tr, ti = orr, oi
        elif 2 * k == n:
            tr, ti = -orr, (None if oi is None else -oi)
        elif 4 * k == n:
            tr, ti = oi, -orr
        else:
            tr = orr * c if oi is None else orr * c + oi * s
            ti = -orr * s if oi is None else oi * c - orr * s
        out.append((plus(er, tr), plus(ei, ti)))
    return out


def plus(a, b):
    if a is None:
        return b
    return a if b is None else a + b


def pick(spectrum, k, n):
    if k <= n // 2:
        return spectrum[k]
    re, im = spectrum[n - k]
    return re, (None if im is None else -im)


def fourier_kernel(
    core_ref, leg_ref, sky_ref, waves_ref, out_ref, send_ref, half_ref, last_ref, x_ref, cos_ref, sin_ref, tail_ref, z_ref, sems
):
    half = half_copy(*PIECES[0][:2], core_ref, leg_ref, half_ref, sems.at[0])
    last = half_copy(*PIECES[2][:2], core_ref, leg_ref, last_ref, sems.at[5])
    copies = [
        pltpu.make_async_copy(sky_ref, x_ref, sems.at[1]),
        pltpu.make_async_copy(waves_ref.at[0:32], cos_ref, sems.at[2]),
        pltpu.make_async_copy(waves_ref.at[32:64], sin_ref, sems.at[3]),
        pltpu.make_async_copy(waves_ref.at[64:320], tail_ref, sems.at[4]),
    ]
    for copy in copies:
        copy.start()
    half.start()
    last.start()
    for copy in copies:
        copy.wait()
    row = lax.broadcasted_iota(jnp.int32, (8, 128), 0)
    total = None
    for r in range(4):
        slabs = []
        for k in range(32):
            maps = [jnp.broadcast_to(x_ref[a, r : r + 1, 128 * k : 128 * k + 128], (8, 128)) for a in range(4)]
            low, high = jnp.where(row < 2, maps[0], maps[1]), jnp.where(row < 6, maps[2], maps[3])
            slabs.append(jnp.where(row < 4, low, high))
        spectrum = real_fft(slabs)
        for m in range(32):
            re, im = pick(spectrum, m, 32)
            c, s = cos_ref[m : m + 1, :], sin_ref[m : m + 1, :]
            if im is None:
                re, im = re * c, -re * s
            else:
                re, im = re * c + im * s, im * c - re * s
            z_ref[8 * m : 8 * m + 8, 0:128] = jnp.where(row % 2 == 0, re, im)
            z_ref[8 * m : 8 * m + 8, 128:256] = jnp.where(row % 2 == 0, im, -re)
        out = jnp.dot(z_ref[...], tail_ref[...], precision=lax.Precision.HIGHEST, preferred_element_type=F32)
        out = pltpu.roll(out, 16 * r, 1) if r else out
        total = out if total is None else total + out
    rounded = (total * (1.0 / 64.0)).astype(BF16)
    out_ref[...] = rounded
    send_ref[...] = rounded
    half.wait()
    last.wait()


def fourier_and_half(core, legendre, sky_maps):
    turn = 2 * np.pi / 4096 * np.outer(np.arange(32), np.arange(128))
    last = 2 * np.pi / 128 * np.outer(np.arange(128), np.arange(16))
    tail = np.zeros((256, 128))
    tail[:128, :16] = np.cos(last)
    tail[128:, :16] = np.sin(last)
    waves = np.concatenate([np.cos(turn), np.sin(turn), tail])
    return kernel_call(
        fourier_kernel,
        55,
        1 << 22,
        out_shape=[jax.ShapeDtypeStruct((256, 128), BF16)] * 2
        + [jax.ShapeDtypeStruct((4, 512, PIECES[k][1]), BF16) for k in (0, 2)],
        in_specs=[SMEM] + [HBM] * 3,
        out_specs=[VMEM] * 4,
        scratch_shapes=[
            pltpu.VMEM((4, 4, 4096), F32),
            pltpu.VMEM((32, 128), F32),
            pltpu.VMEM((32, 128), F32),
            pltpu.VMEM((256, 128), F32),
            pltpu.VMEM((256, 256), F32),
            pltpu.SemaphoreType.DMA((6,)),
        ],
    )(core, legendre, sky_maps, jnp.asarray(waves, F32))


def weights_kernel(core_ref, leg_ref, own_ref, got_ref, *rest):
    out_ref, table_ref, sem = rest[-3:]
    start = pl.multiple_of(core_ref[0] * 1024, 128)
    copy = pltpu.make_async_copy(leg_ref.at[:, :, pl.ds(start, 1024)], table_ref, sem)
    copy.start()
    order_weights(own_ref, got_ref, out_ref)
    copy.wait()


def weights_and_own_half(core, legendre, own_f, got_f, *after):
    return kernel_call(
        weights_kernel,
        42,
        1 << 26,
        out_shape=[jax.ShapeDtypeStruct((16, 256, 256), BF16), jax.ShapeDtypeStruct((4, 512, 1024), BF16)],
        in_specs=[SMEM, HBM, VMEM, VMEM] + [HBM] * len(after),
        out_specs=[VMEM] * 2,
        scratch_shapes=[pltpu.SemaphoreType.DMA],
    )(core, legendre, own_f, got_f, *after)


def order_weights(own_ref, got_ref, out_ref):
    columns = jnp.concatenate([own_ref[...], got_ref[...]], axis=1)
    k = lax.broadcasted_iota(jnp.int32, (256, 256), 0)
    n = lax.broadcasted_iota(jnp.int32, (256, 256), 1)
    cycle_of = jnp.where(k % 128 < 64, (k // 128) * 4 + (k % 128) // 16, -1)
    spread = jnp.where(cycle_of == n // 32, 1.0, 0.0).astype(BF16)
    keep = jnp.where((k // 8) == (n % 32), 1.0, 0.0).astype(BF16)
    for g in range(16):
        pick_group = jnp.where(n % 16 == g, 1.0, 0.0).astype(BF16)
        spread_out = jnp.dot(columns * pick_group, spread, preferred_element_type=F32)
        out_ref[g] = spread_out.astype(BF16) * keep


def slots_along(axis, me):
    out = []
    for d in range(4):
        at = (me + d) % 4
        out.append({X: at * 128, Y: at * 32, Z: at % 2 * 16 + at // 2 * 4}[axis])
    return out


def chip_sums_kernel(first, width, axes, here_ref, owner_ref, weights, table, got_ref, *rest):
    outs, sums = rest[-5:-1], rest[-1]
    core = here_ref[3]
    for g in range(16):
        rows = slice(32 * g, 32 * g + 32)
        own = table[:, rows, first : first + width].reshape(128, width)
        values = jnp.concatenate([own, got_ref[:, rows, :].reshape(128, width)])
        done = jnp.dot(weights[g], values, preferred_element_type=F32)
        sums[rows] = done.astype(BF16).reshape(32, 8, width)
    along = {axis: slots_along(axis, here_ref[k]) for k, axis in enumerate((X, Y, Z))}
    parts = []
    for on_0, on_1 in zip(*axes):
        if on_0 == on_1:
            parts.append(along[on_0])
        else:
            parts.append([jnp.where(core == 0, v0, v1) for v0, v1 in zip(along[on_0], along[on_1])])
    for a in range(4):
        for b in range(4):
            for c in range(4):
                chip = parts[0][a] + parts[1][b] + parts[2][c]
                for q in range(8):
                    slot = chip + q // 4 * 8 + q % 4
                    outs[a][(b * 4 + c) * 8 + q] = sums[owner_ref[slot]]


def chip_sums(piece, here, owner_table, weights, table, got, *after):
    first, width, colour = piece
    return kernel_call(
        functools.partial(chip_sums_kernel, first, width, COLOURS[colour][2]),
        20,
        width * 1_000_000,
        out_shape=[jax.ShapeDtypeStruct((128, 8, width), BF16)] * 4,
        in_specs=[SMEM, SMEM, VMEM, VMEM, VMEM] + [HBM] * len(after),
        out_specs=[VMEM] * 4,
        scratch_shapes=[pltpu.VMEM((512, 8, width), BF16)],
    )(here, owner_table, weights, table, got, *after)


def total_of(refs, part):
    total = refs[0][part].astype(F32)
    for ref in refs[1:]:
        total = total + ref[part].astype(F32)
    return total


def add_kernel(counts, *refs):
    outs = refs[-4:]
    count = outs[0].shape[0]
    for d, out in enumerate(outs):
        part = pl.ds(d * count, count)
        lane, k = 0, 0
        for n in counts:
            total = total_of(refs[k : k + n], part)
            out[:, :, lane : lane + total.shape[2]] = total.astype(out.dtype)
            lane, k = lane + total.shape[2], k + n


def add_blocks(pieces, *after):
    count, rows, _ = pieces[0][0].shape
    width = sum(parts[0].shape[2] for parts in pieces)
    counts = [len(parts) for parts in pieces]
    return kernel_call(
        functools.partial(add_kernel, counts),
        12,
        count * width * 64,
        out_shape=[jax.ShapeDtypeStruct((count // 4, rows, width), F32 if d == 0 else BF16) for d in range(4)],
        in_specs=[VMEM] * sum(counts) + [HBM] * len(after),
        out_specs=[VMEM] * 4,
    )(*[block for parts in pieces for block in parts], *after)


def combine_kernel(a_ref, b_ref, *rest):
    everything = pl.ds(0, a_ref.shape[0])
    rest[-1][...] = total_of((a_ref, b_ref), everything).astype(BF16)


def combine(a, b, *after):
    return kernel_call(
        combine_kernel,
        8,
        a.size,
        out_shape=jax.ShapeDtypeStruct(a.shape, BF16),
        in_specs=[VMEM] * 2 + [HBM] * len(after),
        out_specs=VMEM,
    )(a, b, *after)


def finish_kernel(core_ref, order_ref, *refs):
    ins, (own_ref, send_ref, cross_ref) = refs[:-3], refs[-3:]
    core = core_ref[0]
    for colour, (first, width, _) in enumerate(COLOURS):
        lane = slice(first, first + width)
        ell = lax.broadcasted_iota(jnp.int32, (8, width), 1) + core * 1024 + first
        totals = [jnp.zeros((8, width), F32) for _ in range(4)]
        parts = ins[4 * colour : 4 * colour + 4]

        def slot_sum(slot):
            h = parts[0][slot].astype(F32) + parts[1][slot].astype(F32)
            h = h + parts[2][slot].astype(F32) + parts[3][slot].astype(F32)
            order = order_ref[slot]
            h = jnp.where(ell >= order, h, 0.0)
            weighted = h * jnp.where(order == 0, 1.0, 2.0)
            for delta in range(4):
                other = pltpu.roll(h, 8 - 2 * delta, 0) if delta else h
                totals[delta] = totals[delta] + weighted * other
            return h

        for j in range(4):
            own_ref[j, :, lane] = slot_sum(core * 4 + j)
            send_ref[j, :, lane] = slot_sum((1 - core) * 4 + j)
        here = pl.ds(pl.multiple_of(core * 1024 + first, 128), width)
        there = pl.ds(pl.multiple_of((1 - core) * 1024 + first, 128), width)
        cross_ref[:, there] = jnp.zeros((10, width), F32)
        row = 0
        for i in range(4):
            for j in range(i, 4):
                t = totals[j - i]
                cross_ref[row : row + 1, here] = t[2 * i : 2 * i + 1] + t[2 * i + 1 : 2 * i + 2]
                row += 1


def finish(core, orders, parts):
    return kernel_call(
        finish_kernel,
        4,
        8 * 8 * 1024 * 16,
        out_shape=[
            jax.ShapeDtypeStruct((4, 8, 1024), F32),
            jax.ShapeDtypeStruct((4, 8, 1024), F32),
            jax.ShapeDtypeStruct((10, 2048), F32),
        ],
        in_specs=[SMEM, SMEM] + [VMEM] * len(parts),
        out_specs=[VMEM] * 3,
    )(core, orders, *parts)


def steps(sky_maps, legendre, owner_table):
    my_index = lax.axis_index(BLK_GRP)
    here = places(my_index)
    core = here[CORE]
    core_scalar = core.reshape(1).astype(jnp.int32)

    here_scalars = jnp.stack([here[axis] for axis in (X, Y, Z, CORE)]).astype(jnp.int32)

    own_f, send_f, half, half_2 = fourier_and_half(core_scalar, legendre, sky_maps)
    got_f = swap_cores(send_f)
    got_0 = swap_cores(half)
    half_1 = second_half(core_scalar, legendre)
    got_1 = swap_cores(half_1)
    got_2 = swap_cores(half_2)
    weights, table = weights_and_own_half(core_scalar, legendre, own_f, got_f, half_1)

    def move(block, stage, colour, shift):
        axes = COLOURS[colour][2]
        return shift_along(block, (axes[0][stage], axes[1][stage]), shift)

    def exchange(sent, stage, colour):
        return [sent[0]] + [move(sent[d], stage, colour, d) for d in SHIFTS]

    def sums_of(k, got, *after):
        return chip_sums(PIECES[k], here_scalars, owner_table, weights, table, got, *after)

    up = sums_of(0, got_0)
    through_up, from_above = move(up[2], 0, 0, 1), move(up[3], 0, 0, 3)
    down = sums_of(1, got_1)
    through_down, from_below = move(down[2], 0, 0, 3), move(down[1], 0, 0, 1)
    sent = sums_of(2, got_2, down[0])
    colour_1 = [[sent[0], move(sent[2], 0, 1, 2)]]
    both_up = combine(up[1], through_up, sent[0])
    from_below_up = move(both_up, 0, 0, 1)
    colour_1[0] += [move(sent[d], 0, 1, d) for d in (1, 3)]
    both_down = combine(down[3], through_down, both_up)
    from_above_down = move(both_down, 0, 0, 3)
    colour_0 = [[up[0], from_above, from_below_up], [down[0], from_below, from_above_down]]
    pieces = [colour_0, colour_1]
    after = []
    for stage in (1, 2):
        for colour in (0, 1):
            sent = add_blocks(pieces[colour], *after)
            after = sent[:1]
            pieces[colour] = [exchange(sent, stage, colour)]
    last = pieces[0][0] + pieces[1][0]

    first_slot = index_of({**here, CORE: 0}) * 4
    chip_orders = jnp.concatenate(
        [lax.dynamic_slice_in_dim(owner_table, first_slot + 8 * c, 4) for c in range(2)]
    )
    own, send, cross = finish(core_scalar, chip_orders, last)
    got = swap_cores(send)

    terms = jnp.transpose(cross.reshape(10, 128, 16), (1, 0, 2)).reshape(128, 160)
    power = lax.all_to_all(terms, BLK_GRP, 0, 0, tiled=True)
    power = jnp.sum(power, axis=0).reshape(10, 16)
    ells = my_index * 16 + lax.iota(jnp.int32, 16)
    spectra = power / (2 * ells + 1).astype(F32)[None, :]

    low, high = jnp.where(core == 0, own, got), jnp.where(core == 0, got, own)
    harmonics = jnp.concatenate([low, high], axis=-1)
    harmonics = harmonics.reshape(4, 4, 2, 2048)
    return harmonics, spectra


def solution(mesh):
    finer = Mesh(
        mesh.devices.reshape(4, 4, 2, 2, mesh.shape["grp"]),
        BLK_GRP,
    )
    in_specs = (P(None, BLK_GRP, None), P(BLK_GRP, None, None), P())
    out_specs = (P(BLK_GRP, None, None, None), P(None, BLK_GRP))
    return jax.shard_map(steps, mesh=finer, in_specs=in_specs, out_specs=out_specs, check_vma=False)
```

```python
import functools
import math

import jax
import jax.numpy as jnp
import numpy as np
from jax import lax
from jax.experimental import pallas as pl
from jax.experimental.pallas import tpu as pltpu
from jax.sharding import Mesh
from jax.sharding import PartitionSpec as P


BLK_GRP = ("blk_0", "blk_1", "blk_2", "blk_3", "grp")
X, Y, Z, CORE = "blk_0", "blk_1", "z", "blk_3"
COLOURS = (
    (0, 768, ((X, Y, Z), (Y, Z, X))),
    (768, 256, ((Z, X, Y), (Z, X, Y))),
)
PIECES = ((0, 512, 0), (512, 256, 0), (768, 256, 1))
SHIFTS = (1, 3, 2)
F32, BF16 = jnp.float32, jnp.bfloat16
SMEM = pl.BlockSpec(memory_space=pltpu.SMEM)
VMEM = pl.BlockSpec(memory_space=pltpu.VMEM)
HBM = pl.BlockSpec(memory_space=pltpu.HBM)


def places(device):
    return {
        X: device // 32,
        Y: device // 8 % 4,
        Z: device % 2 * 2 + device // 4 % 2,
        CORE: device // 2 % 2,
    }


def index_of(place):
    z = place[Z]
    return place[X] * 32 + place[Y] * 8 + z % 2 * 4 + place[CORE] * 2 + z // 2


def shift_along(x, axes, shift):
    pairs = []
    for device in range(128):
        place = places(device)
        axis = axes[place[CORE]]
        pairs.append((device, index_of({**place, axis: (place[axis] + shift) % 4})))
    return lax.ppermute(x, BLK_GRP, pairs)


def swap_cores(x):
    return lax.ppermute(x, CORE, [(0, 1), (1, 0)])


def kernel_call(kernel, mib, flops, **kwargs):
    return pl.pallas_call(
        kernel,
        compiler_params=pltpu.CompilerParams(vmem_limit_bytes=mib << 20),
        cost_estimate=pl.CostEstimate(flops=flops, bytes_accessed=1 << 20, transcendentals=0),
        **kwargs,
    )


class Copies:
    def __init__(self, sources, sems, base=0):
        self.copies = [pltpu.make_async_copy(a, b, sems.at[base + k]) for k, (a, b) in enumerate(sources)]

    def start(self):
        for copy in self.copies:
            copy.start()

    def wait(self):
        for copy in self.copies:
            copy.wait()


def columns_copy(start, width, leg_ref, out_ref, sems, base=0):
    return Copies([(leg_ref.at[r, :, pl.ds(start, width)], out_ref.at[r]) for r in range(4)], sems, base)


def half_copy(first, width, core_ref, leg_ref, out_ref, sems, base=0):
    start = pl.multiple_of((1 - core_ref[0]) * 1024 + first, 128)
    return columns_copy(start, width, leg_ref, out_ref, sems, base)


def half_kernel(core_ref, leg_ref, out_ref, sems):
    copy = half_copy(*PIECES[1][:2], core_ref, leg_ref, out_ref, sems)
    copy.start()
    copy.wait()


def second_half(core, legendre):
    return kernel_call(
        half_kernel,
        50,
        1 << 20,
        out_shape=jax.ShapeDtypeStruct((4, 512, PIECES[1][1]), BF16),
        in_specs=[SMEM, HBM],
        out_specs=VMEM,
        scratch_shapes=[pltpu.SemaphoreType.DMA((4,))],
    )(core, legendre)


def real_fft(values):
    n = len(values)
    if n == 1:
        return [(values[0], None)]
    even, odd = real_fft(values[0::2]), real_fft(values[1::2])
    half = n // 2
    out = []
    for k in range(half + 1):
        er, ei = pick(even, k % half, half)
        orr, oi = pick(odd, k % half, half)
        c, s = math.cos(2 * math.pi * k / n), math.sin(2 * math.pi * k / n)
        if k == 0:
            tr, ti = orr, oi
        elif 2 * k == n:
            tr, ti = -orr, (None if oi is None else -oi)
        elif 4 * k == n:
            tr, ti = oi, -orr
        else:
            tr = orr * c if oi is None else orr * c + oi * s
            ti = -orr * s if oi is None else oi * c - orr * s
        out.append((plus(er, tr), plus(ei, ti)))
    return out


def plus(a, b):
    if a is None:
        return b
    return a if b is None else a + b


def pick(spectrum, k, n):
    if k <= n // 2:
        return spectrum[k]
    re, im = spectrum[n - k]
    return re, (None if im is None else -im)


def fourier_kernel(
    core_ref, leg_ref, sky_ref, waves_ref, out_ref, send_ref, half_ref, last_ref, x_ref, cos_ref, sin_ref, tail_ref, z_ref, sems
):
    half = half_copy(*PIECES[0][:2], core_ref, leg_ref, half_ref, sems, 0)
    last = half_copy(*PIECES[2][:2], core_ref, leg_ref, last_ref, sems, 4)
    copies = [
        pltpu.make_async_copy(sky_ref, x_ref, sems.at[8]),
        pltpu.make_async_copy(waves_ref.at[0:32], cos_ref, sems.at[9]),
        pltpu.make_async_copy(waves_ref.at[32:64], sin_ref, sems.at[10]),
        pltpu.make_async_copy(waves_ref.at[64:320], tail_ref, sems.at[11]),
    ]
    for copy in copies:
        copy.start()
    half.start()
    last.start()
    for copy in copies:
        copy.wait()
    row = lax.broadcasted_iota(jnp.int32, (8, 128), 0)
    total = None
    for r in range(4):
        slabs = []
        for k in range(32):
            maps = [jnp.broadcast_to(x_ref[a, r : r + 1, 128 * k : 128 * k + 128], (8, 128)) for a in range(4)]
            low, high = jnp.where(row < 2, maps[0], maps[1]), jnp.where(row < 6, maps[2], maps[3])
            slabs.append(jnp.where(row < 4, low, high))
        spectrum = real_fft(slabs)
        for m in range(32):
            re, im = pick(spectrum, m, 32)
            c, s = cos_ref[m : m + 1, :], sin_ref[m : m + 1, :]
            if im is None:
                re, im = re * c, -re * s
            else:
                re, im = re * c + im * s, im * c - re * s
            z_ref[8 * m : 8 * m + 8, 0:128] = jnp.where(row % 2 == 0, re, im)
            z_ref[8 * m : 8 * m + 8, 128:256] = jnp.where(row % 2 == 0, im, -re)
        out = jnp.dot(z_ref[...], tail_ref[...], precision=lax.Precision.HIGHEST, preferred_element_type=F32)
        out = pltpu.roll(out, 16 * r, 1) if r else out
        total = out if total is None else total + out
    rounded = (total * (1.0 / 64.0)).astype(BF16)
    out_ref[...] = rounded
    send_ref[...] = rounded
    half.wait()
    last.wait()


def fourier_and_half(core, legendre, sky_maps):
    turn = 2 * np.pi / 4096 * np.outer(np.arange(32), np.arange(128))
    last = 2 * np.pi / 128 * np.outer(np.arange(128), np.arange(16))
    tail = np.zeros((256, 128))
    tail[:128, :16] = np.cos(last)
    tail[128:, :16] = np.sin(last)
    waves = np.concatenate([np.cos(turn), np.sin(turn), tail])
    return kernel_call(
        fourier_kernel,
        55,
        1 << 22,
        out_shape=[jax.ShapeDtypeStruct((256, 128), BF16)] * 2
        + [jax.ShapeDtypeStruct((4, 512, PIECES[k][1]), BF16) for k in (0, 2)],
        in_specs=[SMEM] + [HBM] * 3,
        out_specs=[VMEM] * 4,
        scratch_shapes=[
            pltpu.VMEM((4, 4, 4096), F32),
            pltpu.VMEM((32, 128), F32),
            pltpu.VMEM((32, 128), F32),
            pltpu.VMEM((256, 128), F32),
            pltpu.VMEM((256, 256), F32),
            pltpu.SemaphoreType.DMA((12,)),
        ],
    )(core, legendre, sky_maps, jnp.asarray(waves, F32))


def weights_kernel(core_ref, leg_ref, own_ref, got_ref, *rest):
    out_ref, table_ref, sems = rest[-3:]
    start = pl.multiple_of(core_ref[0] * 1024, 128)
    copy = columns_copy(start, 1024, leg_ref, table_ref, sems)
    copy.start()
    order_weights(own_ref, got_ref, out_ref)
    copy.wait()


def weights_and_own_half(core, legendre, own_f, got_f, *after):
    return kernel_call(
        weights_kernel,
        42,
        1 << 26,
        out_shape=[jax.ShapeDtypeStruct((16, 256, 256), BF16), jax.ShapeDtypeStruct((4, 512, 1024), BF16)],
        in_specs=[SMEM, HBM, VMEM, VMEM] + [HBM] * len(after),
        out_specs=[VMEM] * 2,
        scratch_shapes=[pltpu.SemaphoreType.DMA((4,))],
    )(core, legendre, own_f, got_f, *after)


def order_weights(own_ref, got_ref, out_ref):
    columns = jnp.concatenate([own_ref[...], got_ref[...]], axis=1)
    k = lax.broadcasted_iota(jnp.int32, (256, 256), 0)
    n = lax.broadcasted_iota(jnp.int32, (256, 256), 1)
    cycle_of = jnp.where(k % 128 < 64, (k // 128) * 4 + (k % 128) // 16, -1)
    spread = jnp.where(cycle_of == n // 32, 1.0, 0.0).astype(BF16)
    keep = jnp.where((k // 8) == (n % 32), 1.0, 0.0).astype(BF16)
    for g in range(16):
        pick_group = jnp.where(n % 16 == g, 1.0, 0.0).astype(BF16)
        spread_out = jnp.dot(columns * pick_group, spread, preferred_element_type=F32)
        out_ref[g] = spread_out.astype(BF16) * keep


def slots_along(axis, me):
    out = []
    for d in range(4):
        at = (me + d) % 4
        out.append({X: at * 128, Y: at * 32, Z: at % 2 * 16 + at // 2 * 4}[axis])
    return out


def chip_sums_kernel(first, width, axes, here_ref, owner_ref, weights, table, got_ref, *rest):
    outs, sums = rest[-5:-1], rest[-1]
    core = here_ref[3]
    for g in range(16):
        rows = slice(32 * g, 32 * g + 32)
        own = table[:, rows, first : first + width].reshape(128, width)
        values = jnp.concatenate([own, got_ref[:, rows, :].reshape(128, width)])
        done = jnp.dot(weights[g], values, preferred_element_type=F32)
        sums[rows] = done.astype(BF16).reshape(32, 8, width)
    along = {axis: slots_along(axis, here_ref[k]) for k, axis in enumerate((X, Y, Z))}
    parts = []
    for on_0, on_1 in zip(*axes):
        if on_0 == on_1:
            parts.append(along[on_0])
        else:
            parts.append([jnp.where(core == 0, v0, v1) for v0, v1 in zip(along[on_0], along[on_1])])
    for a in range(4):
        for b in range(4):
            for c in range(4):
                chip = parts[0][a] + parts[1][b] + parts[2][c]
                for q in range(8):
                    slot = chip + q // 4 * 8 + q % 4
                    outs[a][(b * 4 + c) * 8 + q] = sums[owner_ref[slot]]


def chip_sums(piece, here, owner_table, weights, table, got, *after):
    first, width, colour = piece
    return kernel_call(
        functools.partial(chip_sums_kernel, first, width, COLOURS[colour][2]),
        20,
        width * 1_000_000,
        out_shape=[jax.ShapeDtypeStruct((128, 8, width), BF16)] * 4,
        in_specs=[SMEM, SMEM, VMEM, VMEM, VMEM] + [HBM] * len(after),
        out_specs=[VMEM] * 4,
        scratch_shapes=[pltpu.VMEM((512, 8, width), BF16)],
    )(here, owner_table, weights, table, got, *after)


def total_of(refs, part):
    total = refs[0][part].astype(F32)
    for ref in refs[1:]:
        total = total + ref[part].astype(F32)
    return total


def add_kernel(counts, *refs):
    outs = refs[-4:]
    count = outs[0].shape[0]
    for d, out in enumerate(outs):
        part = pl.ds(d * count, count)
        lane, k = 0, 0
        for n in counts:
            total = total_of(refs[k : k + n], part)
            out[:, :, lane : lane + total.shape[2]] = total.astype(out.dtype)
            lane, k = lane + total.shape[2], k + n


def add_blocks(pieces, *after):
    count, rows, _ = pieces[0][0].shape
    width = sum(parts[0].shape[2] for parts in pieces)
    counts = [len(parts) for parts in pieces]
    return kernel_call(
        functools.partial(add_kernel, counts),
        12,
        count * width * 64,
        out_shape=[jax.ShapeDtypeStruct((count // 4, rows, width), F32 if d == 0 else BF16) for d in range(4)],
        in_specs=[VMEM] * sum(counts) + [HBM] * len(after),
        out_specs=[VMEM] * 4,
    )(*[block for parts in pieces for block in parts], *after)


def combine_kernel(a_ref, b_ref, *rest):
    everything = pl.ds(0, a_ref.shape[0])
    rest[-1][...] = total_of((a_ref, b_ref), everything).astype(BF16)


def combine(a, b, *after):
    return kernel_call(
        combine_kernel,
        8,
        a.size,
        out_shape=jax.ShapeDtypeStruct(a.shape, BF16),
        in_specs=[VMEM] * 2 + [HBM] * len(after),
        out_specs=VMEM,
    )(a, b, *after)


def finish_kernel(core_ref, order_ref, *refs):
    ins, (own_ref, send_ref, cross_ref) = refs[:-3], refs[-3:]
    core = core_ref[0]
    for colour, (first, width, _) in enumerate(COLOURS):
        lane = slice(first, first + width)
        ell = lax.broadcasted_iota(jnp.int32, (8, width), 1) + core * 1024 + first
        totals = [jnp.zeros((8, width), F32) for _ in range(4)]
        parts = ins[4 * colour : 4 * colour + 4]

        def slot_sum(slot):
            h = parts[0][slot].astype(F32) + parts[1][slot].astype(F32)
            h = h + parts[2][slot].astype(F32) + parts[3][slot].astype(F32)
            order = order_ref[slot]
            h = jnp.where(ell >= order, h, 0.0)
            weighted = h * jnp.where(order == 0, 1.0, 2.0)
            for delta in range(4):
                other = pltpu.roll(h, 8 - 2 * delta, 0) if delta else h
                totals[delta] = totals[delta] + weighted * other
            return h

        for j in range(4):
            own_ref[j, :, lane] = slot_sum(core * 4 + j)
            send_ref[j, :, lane] = slot_sum((1 - core) * 4 + j)
        here = pl.ds(pl.multiple_of(core * 1024 + first, 128), width)
        there = pl.ds(pl.multiple_of((1 - core) * 1024 + first, 128), width)
        cross_ref[:, there] = jnp.zeros((10, width), F32)
        row = 0
        for i in range(4):
            for j in range(i, 4):
                t = totals[j - i]
                cross_ref[row : row + 1, here] = t[2 * i : 2 * i + 1] + t[2 * i + 1 : 2 * i + 2]
                row += 1


def finish(core, orders, parts):
    return kernel_call(
        finish_kernel,
        4,
        8 * 8 * 1024 * 16,
        out_shape=[
            jax.ShapeDtypeStruct((4, 8, 1024), F32),
            jax.ShapeDtypeStruct((4, 8, 1024), F32),
            jax.ShapeDtypeStruct((10, 2048), F32),
        ],
        in_specs=[SMEM, SMEM] + [VMEM] * len(parts),
        out_specs=[VMEM] * 3,
    )(core, orders, *parts)


def steps(sky_maps, legendre, owner_table):
    my_index = lax.axis_index(BLK_GRP)
    here = places(my_index)
    core = here[CORE]
    core_scalar = core.reshape(1).astype(jnp.int32)

    here_scalars = jnp.stack([here[axis] for axis in (X, Y, Z, CORE)]).astype(jnp.int32)

    own_f, send_f, half, half_2 = fourier_and_half(core_scalar, legendre, sky_maps)
    got_f = swap_cores(send_f)
    got_0 = swap_cores(half)
    half_1 = second_half(core_scalar, legendre)
    got_1 = swap_cores(half_1)
    got_2 = swap_cores(half_2)
    weights, table = weights_and_own_half(core_scalar, legendre, own_f, got_f, half_1)

    def move(block, stage, colour, shift):
        axes = COLOURS[colour][2]
        return shift_along(block, (axes[0][stage], axes[1][stage]), shift)

    def exchange(sent, stage, colour):
        return [sent[0]] + [move(sent[d], stage, colour, d) for d in (SHIFTS if stage == 2 else (2, 1, 3))]

    def sums_of(k, got, *after):
        return chip_sums(PIECES[k], here_scalars, owner_table, weights, table, got, *after)

    up = sums_of(0, got_0)
    through_up, from_above = move(up[2], 0, 0, 1), move(up[3], 0, 0, 3)
    down = sums_of(1, got_1)
    through_down, from_below = move(down[2], 0, 0, 3), move(down[1], 0, 0, 1)
    sent = sums_of(2, got_2, down[0])
    colour_1 = [[sent[0], move(sent[2], 0, 1, 2)]]
    both_up = combine(up[1], through_up, sent[0])
    from_below_up = move(both_up, 0, 0, 1)
    colour_1[0] += [move(sent[d], 0, 1, d) for d in (1, 3)]
    both_down = combine(down[3], through_down, both_up)
    from_above_down = move(both_down, 0, 0, 3)
    colour_0 = [[up[0], from_above, from_below_up], [down[0], from_below, from_above_down]]
    pieces = [colour_0, colour_1]
    after = []
    for stage in (1, 2):
        for colour in (0, 1):
            sent = add_blocks(pieces[colour], *after)
            after = sent[:1]
            pieces[colour] = [exchange(sent, stage, colour)]
    last = pieces[0][0] + pieces[1][0]

    first_slot = index_of({**here, CORE: 0}) * 4
    chip_orders = jnp.concatenate(
        [lax.dynamic_slice_in_dim(owner_table, first_slot + 8 * c, 4) for c in range(2)]
    )
    own, send, cross = finish(core_scalar, chip_orders, last)
    got = swap_cores(send)

    terms = jnp.transpose(cross.reshape(10, 128, 16), (1, 0, 2)).reshape(128, 160)
    power = lax.all_to_all(terms, BLK_GRP, 0, 0, tiled=True)
    power = jnp.sum(power, axis=0).reshape(10, 16)
    ells = my_index * 16 + lax.iota(jnp.int32, 16)
    spectra = power / (2 * ells + 1).astype(F32)[None, :]

    low, high = jnp.where(core == 0, own, got), jnp.where(core == 0, got, own)
    harmonics = jnp.concatenate([low, high], axis=-1)
    harmonics = harmonics.reshape(4, 4, 2, 2048)
    return harmonics, spectra


def solution(mesh):
    finer = Mesh(
        mesh.devices.reshape(4, 4, 2, 2, mesh.shape["grp"]),
        BLK_GRP,
    )
    in_specs = (P(None, BLK_GRP, None), P(BLK_GRP, None, None), P())
    out_specs = (P(BLK_GRP, None, None, None), P(None, BLK_GRP))
    return jax.shard_map(steps, mesh=finer, in_specs=in_specs, out_specs=out_specs, check_vma=False)
```
